512 devices in a mesh: out: 8 (over y, core), ctr: 64 (over z, x).
Axes of the slice: x: 4, y: 4, z: 16, core: 2. Of those that a mesh axis runs over, the one named last changes fastest.
Arguments:
- centers: bfloat16 [65536, 1024], P('ctr'), may hold values from -6 to 6
- weights: float32 [65536, 1000], P('ctr', 'out'), may hold values from -1.2 to 1.2
- targets: float32 [512, 1000], P(None, 'out'), may hold values from -6 to 6
- batch_rows: int32 [512], replicated, may hold values from 0 to 65535, as said below
- subsample: int32 [32768], P('ctr'), may hold values from 0 to 65535, as said below
- eigvecs: bfloat16 [32768, 512], P('ctr'), may hold values from -0.25 to 0.25
- eig_scale: float32 [512], replicated, may hold values from 0.05 to 0.5
Outputs:
- updated: float32 [65536, 1000], P('ctr', 'out')
- residual: float32 [512, 1000], P(None, 'out')
The draws below stay inside these ranges and needn't reach their ends.
Inputs may be any that keep to these rules, and one draw needn't show every extreme that they name: `batch_rows`: the entries are distinct. `subsample`: the entries are distinct; the 512 entries of block c (entries c * 512 to (c + 1) * 512 - 1) lie in the center rows c * 1024 to (c + 1) * 1024 - 1.
All inputs are finite; a program needn't handle non-finite values.
Results may differ from the reference program's by a relative error of at most 0.0065.
Values may be sent and summed in bfloat16 or wider, within the bound.
No kernel may reach another device: no remote copies, remote signals or barrier semaphores. Data moves between devices by JAX's collectives and lax.ppermute only.
A program may use at most 64 MiB of HBM per device.

```python
import math
import jax
import jax.numpy as jnp
from jax import lax

D = 1024
L = 1000
Q = 512
M = 512
N_DEV = 1024
S_DEV = 512
N = 65536
S = 32768


def draw_batch_rows(key, part):
    return jax.random.permutation(key, N)[:M].astype(jnp.int32)


def draw_subsample(key, part):

    def draw_block(subkey):
        return jax.random.permutation(subkey, N_DEV)[:S_DEV]
    blocks = N // N_DEV
    chosen = jax.vmap(draw_block)(jax.random.split(key, blocks))
    offsets = jnp.arange(blocks, dtype=jnp.int32)[:, None] * N_DEV
    return (chosen.astype(jnp.int32) + offsets).reshape(-1).astype(jnp.int32)


def shard_levels(key, shape, pieces, least, top_value):
    def one(axis_at, shards_of):
        steps = jax.random.uniform(jax.random.fold_in(jax.random.fold_in(key, 6), axis_at), (shards_of,), jnp.float32, least / len(pieces), top_value / len(pieces))
        return jnp.repeat(jnp.exp(steps), shape[axis_at] // shards_of).reshape((-1,) + (1,) * (len(shape) - axis_at - 1))

    loudness = one(*pieces[0])
    for cut in pieces[1:]:
        loudness = loudness * one(*cut)
    return loudness


def noise(stream_key, shape, deviation, bound, shards=(), held_as=jnp.bfloat16):
    entries = jax.random.normal(stream_key, shape, jnp.float32) * deviation
    if len(shards) > 0:
        entries = shard_levels(stream_key, shape, shards, -0.22, 0.18) * entries
    return jnp.clip(entries, min=-bound, max=bound).astype(held_as)


def setup_inputs(seed: int = 0) -> dict:
    streams_of = jax.random.split(jax.random.key(seed), 8)
    centers = noise(streams_of[0], (N, D), 1.0, 6.0, ((0, 64),))
    weights = noise(streams_of[1], (N, L), 0.2, 1.2, ((0, 64), (1, 8)), jnp.float32)
    targets = noise(streams_of[2], (M, L), 1.0, 6.0, ((1, 8),), jnp.float32)
    batch_rows = draw_batch_rows(jax.random.fold_in(streams_of[7], 71), 0)
    subsample = draw_subsample(jax.random.fold_in(streams_of[7], 71), 0)
    eigvecs = noise(streams_of[5], (S, Q), Q ** -0.5, 0.25, ((0, 64),))
    eig_scale = jnp.clip(jnp.exp(jax.random.uniform(streams_of[6], (Q,), jnp.float32, math.log(0.05), math.log(0.5))), 0.05, 0.5)
    return {"centers": centers, "weights": weights, "targets": targets, "batch_rows": batch_rows, "subsample": subsample, "eigvecs": eigvecs, "eig_scale": eig_scale}


step_size = 0.5


def kernel(left, right):
    left_norm = jnp.sum(jnp.square(left.astype(jnp.float32)), axis=1)
    right_norm = jnp.sum(jnp.square(right.astype(jnp.float32)), axis=1)
    inner_prod = jnp.dot(left, right.T, preferred_element_type=jnp.float32)
    return jnp.exp(-(left_norm[:, None] + right_norm[None, :] - 2.0 * inner_prod) * (2.0 / D))


def reference(centers, weights, targets, batch_rows, subsample, eigvecs, eig_scale):
    batch_feats = centers[batch_rows]
    batch_kernel = kernel(batch_feats, centers).astype(jnp.bfloat16)
    weights_low = weights.astype(jnp.bfloat16)
    prediction = jnp.dot(batch_kernel, weights_low, preferred_element_type=jnp.float32)
    residual = prediction - targets
    sub_feats = centers[subsample]
    sub_kernel = kernel(sub_feats, batch_feats).astype(jnp.bfloat16)
    weighted = jnp.dot(sub_kernel.astype(jnp.float32), residual, precision=lax.Precision.HIGHEST)
    coefficient = jnp.dot(eigvecs.astype(jnp.float32).T, weighted, precision=lax.Precision.HIGHEST)
    correction = jnp.dot(eigvecs.astype(jnp.float32), eig_scale[:, None] * coefficient, precision=lax.Precision.HIGHEST)
    updated = weights.at[batch_rows].add(-step_size * residual)
    updated = updated.at[subsample].add(step_size * correction)
    return updated, residual
```

```python
import jax
import jax.numpy as jnp
from jax import lax
from jax.sharding import Mesh, PartitionSpec as P

step_size = 0.5
OUT = ("y", "core")
CTR = ("z", "x")
LANES = 128


def exchanged(pieces, axes):
    return lax.all_to_all(pieces, axes, split_axis=0, concat_axis=0, tiled=True)


def summed_share(pieces, axes):
    arrived = exchanged(pieces, axes)
    return arrived.astype(jnp.float32).sum(axis=0).astype(jnp.bfloat16)


def copied_to_all(shard, axes):
    return exchanged(jnp.broadcast_to(shard, (lax.axis_size(axes), *shard.shape)), axes)


def shifted(shard, dy, dc):
    ny, ncore = lax.axis_size("y"), lax.axis_size("core")
    if dy == 0 and dc == 0:
        return shard
    pairs = [
        (y * ncore + c, (y + dy) % ny * ncore + (c + dc) % ncore)
        for y in range(ny)
        for c in range(ncore)
    ]
    return lax.ppermute(shard, OUT, pairs)


def by_owner(blocks):
    for dim, name in enumerate(OUT):
        size = lax.axis_size(name)
        back = jnp.concatenate([lax.rev(blocks, (dim,))] * 2, axis=dim)
        start = size - 1 - lax.axis_index(name)
        blocks = lax.dynamic_slice_in_dim(back, start, size, axis=dim)
    return blocks


def one_hot(rows, length):
    return (lax.broadcasted_iota(jnp.int32, (rows.shape[0], length), 1) == rows[:, None]).astype(
        jnp.bfloat16
    )


def one_hot_columns(rows, length):
    return (lax.broadcasted_iota(jnp.int32, (length, rows.shape[0]), 0) == rows[None, :]).astype(
        jnp.bfloat16
    )


def dot(left, right):
    return jnp.dot(left, right, preferred_element_type=jnp.float32)


def summed_over_ctr(block):
    nx, nz = lax.axis_size("x"), lax.axis_size("z")
    width = block.shape[1]
    share = summed_share(block.reshape(nx, nz, width), "x")
    return summed_share(share.reshape(nz, width // LANES, LANES), "z")


def body(centers, weights, targets, batch_rows, subsample, eigvecs, eig_scale):
    low = jnp.bfloat16
    row_count, feature_count = centers.shape
    nout, nx, nz = lax.axis_size(OUT), lax.axis_size("x"), lax.axis_size("z")
    batch = batch_rows.shape[0]
    columns = weights.shape[1]
    block = batch // nout
    ny, ncore = lax.axis_size("y"), lax.axis_size("core")
    base = lax.axis_index(CTR) * row_count
    local_rows = batch_rows - base

    own_rows = lax.dynamic_slice(local_rows, (lax.axis_index(OUT) * block,), (block,))
    picked = dot(one_hot(own_rows, row_count), centers).astype(low)
    share = summed_over_ctr(picked)
    share = copied_to_all(share, "z").reshape(nz, feature_count)
    feats = copied_to_all(share, "x").reshape(block, feature_count)

    weights_low = jnp.pad(weights.astype(low), ((0, 0), (0, LANES - columns)))
    blocks = [shifted(weights_low, dy, dc) for dy in range(ny) for dc in range(ncore)]
    weights_all = jnp.concatenate(blocks, axis=1)

    sub_vecs = dot(one_hot_columns(subsample - base, row_count), eigvecs).astype(low)
    right_norm = jnp.sum(jnp.square(centers.astype(jnp.float32)), axis=1)

    left_norm = jnp.sum(jnp.square(feats.astype(jnp.float32)), axis=1)
    inner = lax.dot_general(
        feats, centers, (((1,), (1,)), ((), ())), preferred_element_type=jnp.float32
    )
    kernel = jnp.exp(
        -(left_norm[:, None] + right_norm[None, :] - 2.0 * inner) * (2.0 / feature_count)
    ).astype(low)

    parts = jnp.concatenate(
        [dot(kernel, weights_all).astype(low), dot(kernel, sub_vecs).astype(low)], axis=1
    )
    share = summed_over_ctr(parts)
    share = copied_to_all(share, "z")
    heads = jnp.moveaxis(share[:, :nout], 1, 0)
    heads = by_owner(heads.reshape(ny, ncore, nz, LANES)).reshape(heads.shape)
    tails = share[:, nout:].reshape(nz, -1)
    pieces = jnp.concatenate(
        [heads, jnp.broadcast_to(tails, (nout, *tails.shape))], axis=2
    )
    pieces = jnp.broadcast_to(pieces[:, None], (nout, nx, *pieces.shape[1:]))
    arrived = exchanged(pieces.reshape(nout * nx, *pieces.shape[2:]), (*OUT, "x"))
    arrived = arrived.reshape(batch, -1)
    residual = arrived[:, :columns].astype(jnp.float32) - targets
    projected = arrived[:, LANES:]
    coefficient = lax.dot_general(
        projected, residual.astype(low), (((0,), (0,)), ((), ())), preferred_element_type=jnp.float32
    )
    changes = jnp.concatenate(
        [(step_size * eig_scale[:, None] * coefficient).astype(low), (-step_size * residual).astype(low)]
    )
    spread = jnp.concatenate([sub_vecs, one_hot_columns(local_rows, row_count)], axis=1)
    updated = weights + dot(spread, changes)
    return (updated, residual)


def solution(mesh):
    axes = ("y", "core", "z", "x")
    fine = Mesh(mesh.devices.reshape(4, 2, 16, 4), axes)
    placed = (P(CTR, None), P(CTR, OUT), P(None, OUT), P(), P(CTR), P(CTR, None), P())
    return jax.shard_map(
        body,
        mesh=fine,
        in_specs=placed,
        out_specs=(P(CTR, OUT), P(None, OUT)),
        check_vma=False,
    )
```

```python
import jax
import jax.numpy as jnp
from jax import lax
from jax.sharding import Mesh, PartitionSpec as P

step_size = 0.5
OUT = ("y", "core")
CTR = ("z", "x")
LANES = 128


def exchanged(pieces, axes):
    return lax.all_to_all(pieces, axes, split_axis=0, concat_axis=0, tiled=True)


def summed_share(pieces, axes):
    arrived = exchanged(pieces, axes)
    return arrived.astype(jnp.float32).sum(axis=0).astype(jnp.bfloat16)


def copied_to_all(shard, axes):
    return exchanged(jnp.broadcast_to(shard, (lax.axis_size(axes), *shard.shape)), axes)


def by_owner(blocks):
    for dim, name in enumerate(OUT):
        size = lax.axis_size(name)
        back = jnp.concatenate([lax.rev(blocks, (dim,))] * 2, axis=dim)
        start = size - 1 - lax.axis_index(name)
        blocks = lax.dynamic_slice_in_dim(back, start, size, axis=dim)
    return blocks


def one_hot(rows, length):
    return (lax.broadcasted_iota(jnp.int32, (rows.shape[0], length), 1) == rows[:, None]).astype(
        jnp.bfloat16
    )


def one_hot_columns(rows, length):
    return (lax.broadcasted_iota(jnp.int32, (length, rows.shape[0]), 0) == rows[None, :]).astype(
        jnp.bfloat16
    )


def dot(left, right):
    return jnp.dot(left, right, preferred_element_type=jnp.float32)


def summed_row(block):
    return summed_share(block.reshape(block.shape[0], -1, LANES), CTR)


def body(centers, weights, targets, batch_rows, subsample, eigvecs, eig_scale):
    low = jnp.bfloat16
    row_count, feature_count = centers.shape
    nout, nx, nz = lax.axis_size(OUT), lax.axis_size("x"), lax.axis_size("z")
    batch = batch_rows.shape[0]
    columns = weights.shape[1]
    block = batch // nout
    ny, ncore = lax.axis_size("y"), lax.axis_size("core")
    base = lax.axis_index(CTR) * row_count
    local_rows = batch_rows - base

    own_rows = lax.dynamic_slice(local_rows, (lax.axis_index(OUT) * block,), (block,))
    picked = dot(one_hot(own_rows, row_count), centers).astype(low)
    share = summed_row(picked)
    feats = copied_to_all(share, CTR).reshape(block, feature_count)

    weights_low = jnp.pad(weights.astype(low), ((0, 0), (0, LANES - columns)))
    other = lax.ppermute(weights_low, "core", [(i, (i + 1) % ncore) for i in range(ncore)])
    pair = jnp.stack([weights_low, other])
    pairs = [pair] + [
        lax.ppermute(pair, "y", [(i, (i + dy) % ny) for i in range(ny)]) for dy in range(1, ny)
    ]
    weights_all = jnp.concatenate([piece for pair in pairs for piece in pair], axis=1)

    sub_vecs = dot(one_hot_columns(subsample - base, row_count), eigvecs).astype(low)
    right_norm = jnp.sum(jnp.square(centers.astype(jnp.float32)), axis=1)

    left_norm = jnp.sum(jnp.square(feats.astype(jnp.float32)), axis=1)
    inner = lax.dot_general(
        feats, centers, (((1,), (1,)), ((), ())), preferred_element_type=jnp.float32
    )
    kernel = jnp.exp(
        -(left_norm[:, None] + right_norm[None, :] - 2.0 * inner) * (2.0 / feature_count)
    ).astype(low)

    parts = jnp.concatenate(
        [dot(kernel, weights_all).astype(low), dot(kernel, sub_vecs).astype(low)], axis=1
    )
    share = copied_to_all(summed_row(parts), "z")
    heads = jnp.moveaxis(share[:, :nout], 1, 0)
    heads = by_owner(heads.reshape(ny, ncore, nz, LANES)).reshape(heads.shape)
    tails = share[:, nout:].reshape(nz, -1)
    pieces = jnp.concatenate(
        [heads, jnp.broadcast_to(tails, (nout, *tails.shape))], axis=2
    )
    pieces = jnp.broadcast_to(pieces[:, None], (nout, nx, *pieces.shape[1:]))
    arrived = exchanged(pieces.reshape(nout * nx, *pieces.shape[2:]), (*OUT, "x"))
    arrived = arrived.reshape(nout, nx, nz, -1).swapaxes(1, 2).reshape(batch, -1)
    residual = arrived[:, :columns].astype(jnp.float32) - targets
    projected = arrived[:, LANES:]
    coefficient = lax.dot_general(
        projected, residual.astype(low), (((0,), (0,)), ((), ())), preferred_element_type=jnp.float32
    )
    changes = jnp.concatenate(
        [(step_size * eig_scale[:, None] * coefficient).astype(low), (-step_size * residual).astype(low)]
    )
    spread = jnp.concatenate([sub_vecs, one_hot_columns(local_rows, row_count)], axis=1)
    updated = weights + dot(spread, changes)
    return (updated, residual)


def solution(mesh):
    axes = ("y", "core", "z", "x")
    fine = Mesh(mesh.devices.reshape(4, 2, 16, 4), axes)
    placed = (P(CTR, None), P(CTR, OUT), P(None, OUT), P(), P(CTR), P(CTR, None), P())
    return jax.shard_map(
        body,
        mesh=fine,
        in_specs=placed,
        out_specs=(P(CTR, OUT), P(None, OUT)),
        check_vma=False,
    )
```

```python
import jax
import jax.numpy as jnp
from jax import lax
from jax.experimental import pallas as pl
from jax.experimental.pallas import tpu as pltpu
from jax.sharding import Mesh, PartitionSpec as P

step_size = 0.5
OUT = ("y", "core")
CTR = ("z", "x")
LANES = 128
ROUND = 3


def exchanged(pieces, axes):
    return lax.all_to_all(pieces, axes, split_axis=0, concat_axis=0, tiled=True)


def copied_to_all(shard, axes):
    return exchanged(jnp.broadcast_to(shard, (lax.axis_size(axes), *shard.shape)), axes)


def one_hot(rows, length):
    return (lax.broadcasted_iota(jnp.int32, (rows.shape[0], length), 1) == rows[:, None]).astype(
        jnp.bfloat16
    )


def one_hot_columns(rows, length):
    return (lax.broadcasted_iota(jnp.int32, (length, rows.shape[0]), 0) == rows[None, :]).astype(
        jnp.bfloat16
    )


def dot(left, right):
    return jnp.dot(left, right, preferred_element_type=jnp.float32)


def by_owner(blocks, dim, name):
    size = lax.axis_size(name)
    back = jnp.concatenate([lax.rev(blocks, (dim,))] * 2, axis=dim)
    return lax.dynamic_slice_in_dim(back, size - 1 - lax.axis_index(name), size, axis=dim)


def products_kernel(feats_ref, centers_ref, norm_ref, mine_ref, other_ref, vecs_ref, out_ref):
    low = jnp.bfloat16
    feats = feats_ref[...]
    wide = feats.astype(jnp.float32)
    left_norm = jnp.sum(wide * wide, axis=1, keepdims=True)
    inner = lax.dot_general(
        feats, centers_ref[...], (((1,), (1,)), ((), ())), preferred_element_type=jnp.float32
    )
    kernel = jnp.exp(
        -(left_norm + norm_ref[...] - 2.0 * inner) * (2.0 / feats.shape[1])
    ).astype(low)
    at = 0
    for blocks in (mine_ref, other_ref):
        for j in range(blocks.shape[0]):
            out_ref[:, at : at + LANES] = dot(kernel, blocks[j]).astype(low)
            at += LANES
    out_ref[:, at:] = dot(kernel, vecs_ref[...]).astype(low)


def products(feats, centers, norm, mine, other, vecs):
    width = (mine.shape[0] + other.shape[0]) * LANES + vecs.shape[1]
    return pl.pallas_call(
        products_kernel,
        out_shape=jax.ShapeDtypeStruct((feats.shape[0], width), jnp.bfloat16),
        in_specs=[pl.BlockSpec(memory_space=pltpu.VMEM)] * 6,
        out_specs=pl.BlockSpec(memory_space=pltpu.VMEM),
        name="products",
    )(feats, centers, norm, mine, other, vecs)


def body(centers, weights, targets, batch_rows, subsample, eigvecs, eig_scale):
    low = jnp.bfloat16
    row_count, feature_count = centers.shape
    nout, nctr = lax.axis_size(OUT), lax.axis_size(CTR)
    nx, nz = lax.axis_size("x"), lax.axis_size("z")
    ny, ncore = lax.axis_size("y"), lax.axis_size("core")
    place, slice_at = lax.axis_index(CTR), lax.axis_index(OUT)
    batch = batch_rows.shape[0]
    columns = weights.shape[1]
    block = batch // nout
    base = place * row_count

    rank = jnp.sum((batch_rows[None, :] < batch_rows[:, None]).astype(jnp.int32), axis=1)
    edges = jnp.arange(nctr, dtype=jnp.int32) * row_count
    start = jnp.sum((batch_rows[None, :] < edges[:, None]).astype(jnp.int32), axis=1)
    stop = jnp.sum((batch_rows[None, :] < edges[:, None] + row_count).astype(jnp.int32), axis=1)
    most = jnp.max(stop - start)
    lead = start + (slice_at - start) % nout
    own_start = jnp.sum((batch_rows < base).astype(jnp.int32))
    own_stop = jnp.sum((batch_rows < base + row_count).astype(jnp.int32))
    own_lead = own_start + (slice_at - own_start) % nout

    def round_of(turn):
        rows = []
        for k in range(ROUND):
            position = own_lead + (turn * ROUND + k) * nout
            row = jnp.sum(jnp.where(rank == position, batch_rows - base, 0))
            row = lax.dynamic_slice(
                centers, (jnp.clip(row, 0, row_count - 1), 0), (1, feature_count)
            )
            rows.append(jnp.where(position < own_stop, row, jnp.zeros_like(row)))
        share = jnp.concatenate(rows).reshape(-1, LANES)
        arrived = copied_to_all(share, CTR).reshape(nctr * ROUND, feature_count)
        steps = turn * ROUND + jnp.arange(ROUND, dtype=jnp.int32)
        positions = lead[:, None] + steps[None, :] * nout
        slots = jnp.where(positions < stop[:, None], positions // nout, -1).reshape(-1)
        return dot(one_hot_columns(slots, block), arrived).astype(low)

    def more(carry):
        return carry[0] * (ROUND * nout) < most

    def next_round(carry):
        return carry[0] + 1, carry[1] + round_of(carry[0])

    feats = round_of(0)
    _, feats = lax.while_loop(more, next_round, (jnp.int32(1), feats))

    weights_low = jnp.pad(weights.astype(low), ((0, 0), (0, LANES - columns)))
    mine = jnp.stack(
        [weights_low]
        + [
            lax.ppermute(weights_low, "y", [(i, (i + dy) % ny) for i in range(ny)])
            for dy in range(1, ny)
        ]
    )
    other = lax.ppermute(mine, "core", [(i, (i + 1) % ncore) for i in range(ncore)])

    sub_vecs = dot(one_hot_columns(subsample - base, row_count), eigvecs).astype(low)
    right_norm = jnp.sum(jnp.square(centers.astype(jnp.float32)), axis=1)
    parts = products(feats, centers, right_norm[None, :], mine, other, sub_vecs)

    blocks = parts.shape[1] // LANES
    arrived = exchanged(parts.reshape(nctr, blocks // 4, 4, LANES), CTR)
    share = arrived.astype(jnp.float32).sum(axis=0).astype(low)
    share = copied_to_all(share, "z").reshape(nz, blocks, LANES)
    heads = jnp.moveaxis(share[:, :nout], 1, 0).reshape(ncore, ny, nz, LANES)
    heads = by_owner(by_owner(heads, 0, "core"), 1, "y")
    heads = jnp.moveaxis(heads, 0, 1).reshape(nout, nz, LANES)
    tails = share[:, nout:].reshape(nz, -1)
    pieces = jnp.concatenate([heads, jnp.broadcast_to(tails, (nout, *tails.shape))], axis=2)
    pieces = jnp.broadcast_to(pieces[:, None], (nout, nx, *pieces.shape[1:]))
    arrived = exchanged(pieces.reshape(nout * nx, *pieces.shape[2:]), (*OUT, "x"))
    arrived = arrived.reshape(batch, -1)

    slot = rank // nout
    line = (rank % nout) * block + (slot % nx) * nz + slot // nx
    to_batch = one_hot(line, batch)
    line_rows = jnp.sum(
        jnp.where(
            lax.broadcasted_iota(jnp.int32, (batch, batch), 0) == line[None, :],
            batch_rows[None, :],
            0,
        ),
        axis=1,
    )
    line_targets = lax.dot_general(
        to_batch.astype(jnp.float32),
        targets,
        (((0,), (0,)), ((), ())),
        precision=lax.Precision.HIGHEST,
    )
    spread = jnp.concatenate([sub_vecs, one_hot_columns(line_rows - base, row_count)], axis=1)

    line_prediction = arrived[:, :columns]
    line_residual = line_prediction.astype(jnp.float32) - line_targets
    coefficient = lax.dot_general(
        arrived[:, LANES:],
        line_residual.astype(low),
        (((0,), (0,)), ((), ())),
        preferred_element_type=jnp.float32,
    )
    changes = jnp.concatenate(
        [
            (step_size * eig_scale[:, None] * coefficient).astype(low),
            (-step_size * line_residual).astype(low),
        ]
    )
    updated = weights + dot(spread, changes)
    residual = dot(to_batch, line_prediction) - targets
    return (updated, residual)


def solution(mesh):
    axes = ("y", "core", "z", "x")
    fine = Mesh(mesh.devices.reshape(4, 2, 16, 4), axes)
    placed = (P(CTR, None), P(CTR, OUT), P(None, OUT), P(), P(CTR), P(CTR, None), P())
    return jax.shard_map(
        body,
        mesh=fine,
        in_specs=placed,
        out_specs=(P(CTR, OUT), P(None, OUT)),
        check_vma=False,
    )
```

```python
import functools
import jax
import jax.numpy as jnp
from jax import lax
from jax.experimental import pallas as pl
from jax.experimental.pallas import tpu as pltpu
from jax.sharding import Mesh, PartitionSpec as P

step_size = 0.5
OUT = ("y", "core")
CTR = ("z", "x")
LANES = 128
ROUND = 3


def exchanged(pieces, axes):
    return lax.all_to_all(pieces, axes, split_axis=0, concat_axis=0, tiled=True)


def copied_to_all(shard, axes):
    return exchanged(jnp.broadcast_to(shard, (lax.axis_size(axes), *shard.shape)), axes)


def one_hot(rows, length):
    return (lax.broadcasted_iota(jnp.int32, (rows.shape[0], length), 1) == rows[:, None]).astype(
        jnp.bfloat16
    )


def one_hot_columns(rows, length):
    return (lax.broadcasted_iota(jnp.int32, (length, rows.shape[0]), 0) == rows[None, :]).astype(
        jnp.bfloat16
    )


def dot(left, right):
    return jnp.dot(left, right, preferred_element_type=jnp.float32)


def by_owner(blocks, dim, name):
    size = lax.axis_size(name)
    back = jnp.concatenate([lax.rev(blocks, (dim,))] * 2, axis=dim)
    return lax.dynamic_slice_in_dim(back, size - 1 - lax.axis_index(name), size, axis=dim)


def whole(kernel, shape, count):
    vmem = pl.BlockSpec(memory_space=pltpu.VMEM)
    return pl.pallas_call(
        kernel,
        out_shape=shape,
        in_specs=[pl.BlockSpec(memory_space=pltpu.SMEM)] + [vmem] * count,
        out_specs=vmem,
        compiler_params=pltpu.CompilerParams(vmem_limit_bytes=12 << 20),
    )


def rows_below(rows, edge):
    return jnp.sum((rows < edge).astype(jnp.float32), axis=1, keepdims=True).astype(jnp.int32)


def pick_kernel(at_ref, rows_ref, centers_ref, out_ref):
    count = centers_ref.shape[0]
    base, slice_at, step, nout = at_ref[0] * count, at_ref[1], at_ref[2], at_ref[3]
    rows = rows_ref[...]
    here = lax.broadcasted_iota(jnp.int32, (count, 1), 0) + base
    start = rows_below(rows, jnp.full((1, 1), base, jnp.int32))
    lead = start + ((slice_at - start) & (nout - 1))
    held = jnp.sum((rows == here).astype(jnp.float32), axis=1, keepdims=True) > 0
    position = jnp.where(held, rows_below(rows, here), -1)
    steps = lax.broadcasted_iota(jnp.int32, (1, LANES), 1)
    wanted = jnp.where(steps < ROUND, lead + (steps + step) * nout, -2)
    pick = (position == wanted).astype(jnp.float32).astype(jnp.bfloat16)
    found = lax.dot_general(
        pick, centers_ref[...], (((0,), (0,)), ((), ())), preferred_element_type=jnp.float32
    )
    out_ref[...] = found[: out_ref.shape[0]].astype(jnp.bfloat16)


def slot_kernel(at_ref, rows_ref, arrived_ref, out_ref, *, count):
    slice_at, step, nout = at_ref[1], at_ref[2], at_ref[3]
    rows = rows_ref[...]
    line = lax.broadcasted_iota(jnp.int32, (arrived_ref.shape[0], 1), 0)
    scale = (1 << 16) // ROUND + 1
    place = (line * scale) >> 16
    start = rows_below(rows, place * count)
    stop = rows_below(rows, place * count + count)
    lead = start + ((slice_at - start) & (nout - 1))
    position = lead + (line - place * ROUND + step) * nout
    slots = lax.broadcasted_iota(jnp.int32, (1, LANES), 1) * nout + slice_at
    fits = (jnp.where(position < stop, position, -1) == slots).astype(jnp.float32)
    feats = lax.dot_general(
        fits.astype(jnp.bfloat16),
        arrived_ref[...],
        (((0,), (0,)), ((), ())),
        preferred_element_type=jnp.float32,
    )
    out_ref[...] = feats[: out_ref.shape[0]].astype(jnp.bfloat16)


def products_kernel(at_ref, feats_ref, centers_ref, norm_ref, mine_ref, other_ref, vecs_ref, out_ref):
    del at_ref
    low = jnp.bfloat16
    feats = feats_ref[...]
    wide = feats.astype(jnp.float32)
    left_norm = jnp.sum(wide * wide, axis=1, keepdims=True)
    inner = lax.dot_general(
        feats, centers_ref[...], (((1,), (1,)), ((), ())), preferred_element_type=jnp.float32
    )
    kernel = jnp.exp(
        -(left_norm + norm_ref[...] - 2.0 * inner) * (2.0 / feats.shape[1])
    ).astype(low)
    at = 0
    for blocks in (mine_ref, other_ref):
        for j in range(blocks.shape[0]):
            out_ref[:, at : at + LANES] = dot(kernel, blocks[j]).astype(low)
            at += LANES
    out_ref[:, at:] = dot(kernel, vecs_ref[...]).astype(low)


def products(at, feats, centers, norm, mine, other, vecs):
    width = (mine.shape[0] + other.shape[0]) * LANES + vecs.shape[1]
    shape = jax.ShapeDtypeStruct((feats.shape[0], width), jnp.bfloat16)
    return whole(products_kernel, shape, 6)(
        at, feats, centers, norm, mine, other, vecs
    )


def body(centers, weights, targets, batch_rows, subsample, eigvecs, eig_scale):
    low = jnp.bfloat16
    row_count, feature_count = centers.shape
    nout, nctr = lax.axis_size(OUT), lax.axis_size(CTR)
    nx, nz = lax.axis_size("x"), lax.axis_size("z")
    ny, ncore = lax.axis_size("y"), lax.axis_size("core")
    place, slice_at = lax.axis_index(CTR), lax.axis_index(OUT)
    batch = batch_rows.shape[0]
    columns = weights.shape[1]
    block = batch // nout
    base = place * row_count

    edges = jnp.arange(nctr, dtype=jnp.int32)[:, None] * row_count
    owned = (batch_rows[None, :] >= edges) & (batch_rows[None, :] < edges + row_count)
    most = jnp.max(jnp.sum(owned.astype(jnp.int32), axis=1))
    batch_line = batch_rows[None, :]

    def places(turn):
        return jnp.stack([place, slice_at, jnp.int32(turn * ROUND), jnp.int32(nout)])

    def round_of(turn):
        at = places(turn)
        shape = jax.ShapeDtypeStruct((ROUND, feature_count), low)
        share = whole(pick_kernel, shape, 2)(at, batch_line, centers)
        arrived = copied_to_all(share.reshape(-1, LANES), CTR)
        arrived = arrived.reshape(nctr * ROUND, feature_count)
        shape = jax.ShapeDtypeStruct((block, feature_count), low)
        slot = functools.partial(slot_kernel, count=row_count)
        return whole(slot, shape, 2)(at, batch_line, arrived)

    def more(carry):
        return carry[0] * (ROUND * nout) < most

    def next_round(carry):
        return carry[0] + 1, carry[1] + round_of(carry[0])

    feats = round_of(0)
    _, feats = lax.while_loop(more, next_round, (jnp.int32(1), feats))

    weights_low = jnp.pad(weights.astype(low), ((0, 0), (0, LANES - columns)))
    mine = jnp.stack(
        [weights_low]
        + [
            lax.ppermute(weights_low, "y", [(i, (i + dy) % ny) for i in range(ny)])
            for dy in range(1, ny)
        ]
    )
    other = lax.ppermute(mine, "core", [(i, (i + 1) % ncore) for i in range(ncore)])

    sub_vecs = dot(one_hot_columns(subsample - base, row_count), eigvecs).astype(low)
    right_norm = jnp.sum(jnp.square(centers.astype(jnp.float32)), axis=1)
    parts = products(places(0), feats, centers, right_norm[None, :], mine, other, sub_vecs)

    blocks = parts.shape[1] // LANES
    arrived = exchanged(parts.reshape(nctr, blocks // 4, 4, LANES), CTR)
    share = arrived.astype(jnp.float32).sum(axis=0).astype(low)
    share = copied_to_all(share, "z").reshape(nz, blocks, LANES)
    heads = jnp.moveaxis(share[:, :nout], 1, 0).reshape(ncore, ny, nz, LANES)
    heads = by_owner(by_owner(heads, 0, "core"), 1, "y")
    heads = jnp.moveaxis(heads, 0, 1).reshape(nout, nz, LANES)
    tails = share[:, nout:].reshape(nz, -1)
    pieces = jnp.concatenate([heads, jnp.broadcast_to(tails, (nout, *tails.shape))], axis=2)
    pieces = jnp.broadcast_to(pieces[:, None], (nout, nx, *pieces.shape[1:]))
    arrived = exchanged(pieces.reshape(nout * nx, *pieces.shape[2:]), (*OUT, "x"))
    arrived = arrived.reshape(batch, -1)

    rank = jnp.sum((batch_rows[None, :] < batch_rows[:, None]).astype(jnp.int32), axis=1)
    slot = rank // nout
    line = (rank % nout) * block + (slot % nx) * nz + slot // nx
    to_batch = one_hot(line, batch)
    line_rows = jnp.sum(
        jnp.where(
            lax.broadcasted_iota(jnp.int32, (batch, batch), 0) == line[None, :],
            batch_rows[None, :],
            0,
        ),
        axis=1,
    )
    line_targets = lax.dot_general(
        to_batch.astype(jnp.float32),
        targets,
        (((0,), (0,)), ((), ())),
        precision=lax.Precision.HIGHEST,
    )
    batch_spread = one_hot_columns(line_rows - base, row_count)
    line_targets, batch_spread = lax.optimization_barrier((line_targets, batch_spread))
    spread = jnp.concatenate([sub_vecs, batch_spread], axis=1)

    line_prediction = arrived[:, :columns]
    line_residual = line_prediction.astype(jnp.float32) - line_targets
    coefficient = lax.dot_general(
        arrived[:, LANES:],
        line_residual.astype(low),
        (((0,), (0,)), ((), ())),
        preferred_element_type=jnp.float32,
    )
    changes = jnp.concatenate(
        [
            (step_size * eig_scale[:, None] * coefficient).astype(low),
            (-step_size * line_residual).astype(low),
        ]
    )
    updated = weights + dot(spread, changes)
    residual = dot(to_batch, line_prediction) - targets
    return (updated, residual)


def solution(mesh):
    axes = ("y", "core", "z", "x")
    fine = Mesh(mesh.devices.reshape(4, 2, 16, 4), axes)
    placed = (P(CTR, None), P(CTR, OUT), P(None, OUT), P(), P(CTR), P(CTR, None), P())
    return jax.shard_map(
        body,
        mesh=fine,
        in_specs=placed,
        out_specs=(P(CTR, OUT), P(None, OUT)),
        check_vma=False,
    )
```

```python
import functools
import jax
import jax.numpy as jnp
from jax import lax
from jax.experimental import pallas as pl
from jax.experimental.pallas import tpu as pltpu
from jax.sharding import Mesh, PartitionSpec as P

step_size = 0.5
OUT = ("y", "core")
CTR = ("z", "x")
LANES = 128
ROUND = 3


def exchanged(pieces, axes):
    return lax.all_to_all(pieces, axes, split_axis=0, concat_axis=0, tiled=True)


def copied_to_all(shard, axes):
    return exchanged(jnp.broadcast_to(shard, (lax.axis_size(axes), *shard.shape)), axes)


def one_hot(rows, length):
    return (lax.broadcasted_iota(jnp.int32, (rows.shape[0], length), 1) == rows[:, None]).astype(
        jnp.bfloat16
    )


def one_hot_columns(rows, length):
    return (lax.broadcasted_iota(jnp.int32, (length, rows.shape[0]), 0) == rows[None, :]).astype(
        jnp.bfloat16
    )


def dot(left, right):
    return jnp.dot(left, right, preferred_element_type=jnp.float32)


def by_owner(blocks, dim, name):
    size = lax.axis_size(name)
    back = jnp.concatenate([lax.rev(blocks, (dim,))] * 2, axis=dim)
    return lax.dynamic_slice_in_dim(back, size - 1 - lax.axis_index(name), size, axis=dim)


def whole(kernel, shape, count):
    vmem = pl.BlockSpec(memory_space=pltpu.VMEM)
    return pl.pallas_call(
        kernel,
        out_shape=shape,
        in_specs=[pl.BlockSpec(memory_space=pltpu.SMEM)] + [vmem] * count,
        out_specs=jax.tree.map(lambda _: vmem, shape),
        compiler_params=pltpu.CompilerParams(vmem_limit_bytes=12 << 20),
    )


def rows_below(rows, edge):
    return jnp.sum((rows < edge).astype(jnp.float32), axis=1, keepdims=True).astype(jnp.int32)


def pick_kernel(at_ref, rows_ref, centers_ref, out_ref):
    count = centers_ref.shape[0]
    base, slice_at, step, nout = at_ref[0] * count, at_ref[1], at_ref[2], at_ref[3]
    rows = rows_ref[...]
    here = lax.broadcasted_iota(jnp.int32, (count, 1), 0) + base
    start = rows_below(rows, jnp.full((1, 1), base, jnp.int32))
    lead = start + ((slice_at - start) & (nout - 1))
    held = jnp.sum((rows == here).astype(jnp.float32), axis=1, keepdims=True) > 0
    position = jnp.where(held, rows_below(rows, here), -1)
    steps = lax.broadcasted_iota(jnp.int32, (1, LANES), 1)
    wanted = jnp.where(steps < ROUND, lead + (steps + step) * nout, -2)
    pick = (position == wanted).astype(jnp.float32).astype(jnp.bfloat16)
    found = lax.dot_general(
        pick, centers_ref[...], (((0,), (0,)), ((), ())), preferred_element_type=jnp.float32
    )
    out_ref[...] = found[: out_ref.shape[0]].astype(jnp.bfloat16)


def slot_kernel(at_ref, rows_ref, arrived_ref, out_ref, *, count, nx, nz):
    slice_at, step, nout = at_ref[1], at_ref[2], at_ref[3]
    rows = rows_ref[...]
    line = lax.broadcasted_iota(jnp.int32, (arrived_ref.shape[0], 1), 0)
    scale = (1 << 16) // ROUND + 1
    source = (line * scale) >> 16
    place = (source & (nz - 1)) * nx + (source >> (nz.bit_length() - 1))
    start = rows_below(rows, place * count)
    stop = rows_below(rows, place * count + count)
    lead = start + ((slice_at - start) & (nout - 1))
    position = lead + (line - source * ROUND + step) * nout
    slots = lax.broadcasted_iota(jnp.int32, (1, LANES), 1) * nout + slice_at
    fits = (jnp.where(position < stop, position, -1) == slots).astype(jnp.float32)
    feats = lax.dot_general(
        fits.astype(jnp.bfloat16),
        arrived_ref[...],
        (((0,), (0,)), ((), ())),
        preferred_element_type=jnp.float32,
    )
    out_ref[...] = feats[: out_ref.shape[0]].astype(jnp.bfloat16)


def products_kernel(at_ref, feats_ref, centers_ref, norm_ref, mine_ref, other_ref, vecs_ref, out_ref):
    del at_ref
    low = jnp.bfloat16
    feats = feats_ref[...]
    wide = feats.astype(jnp.float32)
    left_norm = jnp.sum(wide * wide, axis=1, keepdims=True)
    inner = lax.dot_general(
        feats, centers_ref[...], (((1,), (1,)), ((), ())), preferred_element_type=jnp.float32
    )
    kernel = jnp.exp(
        -(left_norm + norm_ref[...] - 2.0 * inner) * (2.0 / feats.shape[1])
    ).astype(low)
    at = 0
    for blocks in (mine_ref, other_ref):
        for j in range(blocks.shape[0]):
            out_ref[:, at : at + LANES] = dot(kernel, blocks[j]).astype(low)
            at += LANES
    out_ref[:, at:] = dot(kernel, vecs_ref[...]).astype(low)


def products(at, feats, centers, norm, mine, other, vecs):
    width = (mine.shape[0] + other.shape[0]) * LANES + vecs.shape[1]
    shape = jax.ShapeDtypeStruct((feats.shape[0], width), jnp.bfloat16)
    return whole(products_kernel, shape, 6)(
        at, feats, centers, norm, mine, other, vecs
    )


def tail_kernel(
    at_ref,
    arrived_ref,
    line_targets_ref,
    sub_vecs_ref,
    batch_spread_ref,
    to_batch_ref,
    scale_ref,
    weights_ref,
    targets_ref,
    updated_ref,
    residual_ref,
):
    del at_ref
    low = jnp.bfloat16
    columns = weights_ref.shape[1]
    prediction = arrived_ref[:, :LANES][:, :columns]
    residual = prediction.astype(jnp.float32) - line_targets_ref[...]
    coefficient = lax.dot_general(
        arrived_ref[:, LANES:],
        residual.astype(low),
        (((0,), (0,)), ((), ())),
        preferred_element_type=jnp.float32,
    )
    correction = (step_size * scale_ref[...] * coefficient).astype(low)
    updated_ref[...] = (
        weights_ref[...]
        + dot(sub_vecs_ref[...], correction)
        + dot(batch_spread_ref[...], (-step_size * residual).astype(low))
    )
    residual_ref[...] = dot(to_batch_ref[...], prediction) - targets_ref[...]


def body(centers, weights, targets, batch_rows, subsample, eigvecs, eig_scale):
    low = jnp.bfloat16
    row_count, feature_count = centers.shape
    nout, nctr = lax.axis_size(OUT), lax.axis_size(CTR)
    nx, nz = lax.axis_size("x"), lax.axis_size("z")
    ny, ncore = lax.axis_size("y"), lax.axis_size("core")
    place, slice_at = lax.axis_index(CTR), lax.axis_index(OUT)
    batch = batch_rows.shape[0]
    columns = weights.shape[1]
    block = batch // nout
    base = place * row_count

    edges = jnp.arange(nctr, dtype=jnp.int32)[:, None] * row_count
    owned = (batch_rows[None, :] >= edges) & (batch_rows[None, :] < edges + row_count)
    most = jnp.max(jnp.sum(owned.astype(jnp.int32), axis=1))
    batch_line = batch_rows[None, :]

    def places(turn):
        return jnp.stack([place, slice_at, jnp.int32(turn * ROUND), jnp.int32(nout)])

    def round_of(turn):
        at = places(turn)
        shape = jax.ShapeDtypeStruct((ROUND, feature_count), low)
        share = whole(pick_kernel, shape, 2)(at, batch_line, centers)
        arrived = copied_to_all(share.reshape(-1, LANES), "z")
        arrived = copied_to_all(arrived.reshape(-1, LANES), "x")
        arrived = arrived.reshape(nctr * ROUND, feature_count)
        shape = jax.ShapeDtypeStruct((block, feature_count), low)
        slot = functools.partial(slot_kernel, count=row_count, nx=nx, nz=nz)
        return whole(slot, shape, 2)(at, batch_line, arrived)

    def more(carry):
        return carry[0] * (ROUND * nout) < most

    def next_round(carry):
        return carry[0] + 1, carry[1] + round_of(carry[0])

    feats = round_of(0)
    _, feats = lax.while_loop(more, next_round, (jnp.int32(1), feats))

    weights_low = jnp.pad(weights.astype(low), ((0, 0), (0, LANES - columns)))
    ahead = [(i, (i + 1) % ny) for i in range(ny)]
    back = [(i, (i - 1) % ny) for i in range(ny)]
    one, three = lax.ppermute(weights_low, "y", ahead), lax.ppermute(weights_low, "y", back)
    half = row_count // 2
    two = jnp.concatenate(
        [lax.ppermute(one[:half], "y", ahead), lax.ppermute(three[half:], "y", back)]
    )
    mine = jnp.stack([weights_low, one, two, three])
    other = lax.ppermute(mine, "core", [(i, (i + 1) % ncore) for i in range(ncore)])

    sub_vecs = dot(one_hot_columns(subsample - base, row_count), eigvecs).astype(low)
    right_norm = jnp.sum(jnp.square(centers.astype(jnp.float32)), axis=1)
    parts = products(places(0), feats, centers, right_norm[None, :], mine, other, sub_vecs)

    blocks = parts.shape[1] // LANES
    arrived = exchanged(parts.reshape(nx, nz, parts.shape[1]), "x")
    share = arrived.astype(jnp.float32).sum(axis=0).astype(low)
    arrived = exchanged(share.reshape(nz, blocks // 4, 4, LANES), "z")
    share = arrived.astype(jnp.float32).sum(axis=0).astype(low)
    share = copied_to_all(share, "z").reshape(nz, blocks, LANES)
    heads = jnp.moveaxis(share[:, :nout], 1, 0).reshape(ncore, ny, nz, LANES)
    heads = by_owner(by_owner(heads, 0, "core"), 1, "y")
    heads = jnp.moveaxis(heads, 0, 1).reshape(nout, nz, LANES)
    tails = share[:, nout:].reshape(nz, -1)
    pieces = jnp.concatenate([heads, jnp.broadcast_to(tails, (nout, *tails.shape))], axis=2)
    pieces = jnp.broadcast_to(pieces[:, None], (nout, nx, *pieces.shape[1:]))
    arrived = exchanged(pieces.reshape(nout * nx, *pieces.shape[2:]), (*OUT, "x"))
    arrived = arrived.reshape(batch, -1)

    rank = jnp.sum((batch_rows[None, :] < batch_rows[:, None]).astype(jnp.int32), axis=1)
    line = (rank % nout) * block + rank // nout
    to_batch = one_hot(line, batch)
    line_rows = jnp.sum(
        jnp.where(
            lax.broadcasted_iota(jnp.int32, (batch, batch), 0) == line[None, :],
            batch_rows[None, :],
            0,
        ),
        axis=1,
    )
    line_targets = lax.dot_general(
        to_batch.astype(jnp.float32),
        targets,
        (((0,), (0,)), ((), ())),
        precision=lax.Precision.HIGHEST,
    )
    batch_spread = one_hot_columns(line_rows - base, row_count)
    shapes = (
        jax.ShapeDtypeStruct(weights.shape, jnp.float32),
        jax.ShapeDtypeStruct(targets.shape, jnp.float32),
    )
    return whole(tail_kernel, shapes, 8)(
        places(0),
        arrived,
        line_targets,
        sub_vecs,
        batch_spread,
        to_batch,
        eig_scale[:, None],
        weights,
        targets,
    )


def solution(mesh):
    axes = ("y", "core", "z", "x")
    fine = Mesh(mesh.devices.reshape(4, 2, 16, 4), axes)
    placed = (P(CTR, None), P(CTR, OUT), P(None, OUT), P(), P(CTR), P(CTR, None), P())
    return jax.shard_map(
        body,
        mesh=fine,
        in_specs=placed,
        out_specs=(P(CTR, OUT), P(None, OUT)),
        check_vma=False,
    )
```

```python
import functools
import jax
import jax.numpy as jnp
from jax import lax
from jax.experimental import pallas as pl
from jax.experimental.pallas import tpu as pltpu
from jax.sharding import Mesh, PartitionSpec as P

step_size = 0.5
OUT = ("y", "core")
CTR = ("z", "x")
LANES = 128
ROUND = 3


def exchanged(pieces, axes):
    return lax.all_to_all(pieces, axes, split_axis=0, concat_axis=0, tiled=True)


def copied_to_all(shard, axes):
    return exchanged(jnp.broadcast_to(shard, (lax.axis_size(axes), *shard.shape)), axes)


def one_hot_columns(rows, length):
    return (lax.broadcasted_iota(jnp.int32, (length, rows.shape[0]), 0) == rows[None, :]).astype(
        jnp.bfloat16
    )


def dot(left, right):
    return jnp.dot(left, right, preferred_element_type=jnp.float32)


def by_owner(blocks, dim, name):
    size = lax.axis_size(name)
    back = jnp.concatenate([lax.rev(blocks, (dim,))] * 2, axis=dim)
    return lax.dynamic_slice_in_dim(back, size - 1 - lax.axis_index(name), size, axis=dim)


def whole(kernel, shape, count):
    vmem = pl.BlockSpec(memory_space=pltpu.VMEM)
    return pl.pallas_call(
        kernel,
        out_shape=shape,
        in_specs=[pl.BlockSpec(memory_space=pltpu.SMEM)] + [vmem] * count,
        out_specs=jax.tree.map(lambda _: vmem, shape),
        compiler_params=pltpu.CompilerParams(vmem_limit_bytes=12 << 20),
    )


def rows_below(rows, edge):
    return jnp.sum((rows < edge).astype(jnp.float32), axis=1, keepdims=True).astype(jnp.int32)


def pick_kernel(at_ref, rows_ref, centers_ref, out_ref):
    count = centers_ref.shape[0]
    base, slice_at, step, nout = at_ref[0] * count, at_ref[1], at_ref[2], at_ref[3]
    rows = rows_ref[...]
    here = lax.broadcasted_iota(jnp.int32, (count, 1), 0) + base
    start = rows_below(rows, jnp.full((1, 1), base, jnp.int32))
    lead = start + ((slice_at - start) & (nout - 1))
    held = jnp.sum((rows == here).astype(jnp.float32), axis=1, keepdims=True) > 0
    position = jnp.where(held, rows_below(rows, here), -1)
    steps = lax.broadcasted_iota(jnp.int32, (1, LANES), 1)
    wanted = jnp.where(steps < ROUND, lead + (steps + step) * nout, -2)
    pick = (position == wanted).astype(jnp.float32).astype(jnp.bfloat16)
    found = lax.dot_general(
        pick, centers_ref[...], (((0,), (0,)), ((), ())), preferred_element_type=jnp.float32
    )
    out_ref[...] = found[: out_ref.shape[0]].astype(jnp.bfloat16)


def slot_kernel(at_ref, rows_ref, arrived_ref, out_ref, *, count):
    slice_at, step, nout = at_ref[1], at_ref[2], at_ref[3]
    rows = rows_ref[...]
    line = lax.broadcasted_iota(jnp.int32, (arrived_ref.shape[0], 1), 0)
    scale = (1 << 16) // ROUND + 1
    place = (line * scale) >> 16
    start = rows_below(rows, place * count)
    stop = rows_below(rows, place * count + count)
    lead = start + ((slice_at - start) & (nout - 1))
    position = lead + (line - place * ROUND + step) * nout
    slots = lax.broadcasted_iota(jnp.int32, (1, LANES), 1) * nout + slice_at
    fits = (jnp.where(position < stop, position, -1) == slots).astype(jnp.float32)
    feats = lax.dot_general(
        fits.astype(jnp.bfloat16),
        arrived_ref[...],
        (((0,), (0,)), ((), ())),
        preferred_element_type=jnp.float32,
    )
    out_ref[...] = feats[: out_ref.shape[0]].astype(jnp.bfloat16)


def products_kernel(at_ref, feats_ref, centers_ref, norm_ref, mine_ref, other_ref, vecs_ref, out_ref):
    del at_ref
    low = jnp.bfloat16
    feats = feats_ref[...]
    wide = feats.astype(jnp.float32)
    left_norm = jnp.sum(wide * wide, axis=1, keepdims=True)
    inner = lax.dot_general(
        feats, centers_ref[...], (((1,), (1,)), ((), ())), preferred_element_type=jnp.float32
    )
    kernel = jnp.exp(
        -(left_norm + norm_ref[...] - 2.0 * inner) * (2.0 / feats.shape[1])
    ).astype(low)
    at = 0
    for blocks in (mine_ref, other_ref):
        for j in range(blocks.shape[0]):
            out_ref[:, at : at + LANES] = dot(kernel, blocks[j]).astype(low)
            at += LANES
    out_ref[:, at:] = dot(kernel, vecs_ref[...]).astype(low)


def products(at, feats, centers, norm, mine, other, vecs):
    width = (mine.shape[0] + other.shape[0]) * LANES + vecs.shape[1]
    shape = jax.ShapeDtypeStruct((feats.shape[0], width), jnp.bfloat16)
    return whole(products_kernel, shape, 6)(
        at, feats, centers, norm, mine, other, vecs
    )


def tail_kernel(
    at_ref,
    arrived_ref,
    line_ref,
    scale_ref,
    sub_vecs_ref,
    batch_spread_ref,
    weights_ref,
    targets_ref,
    updated_ref,
    residual_ref,
):
    del at_ref
    low = jnp.bfloat16
    columns = weights_ref.shape[1]
    count, ranks = line_ref.shape[1], scale_ref.shape[1]
    to_line = (lax.broadcasted_iota(jnp.int32, (count, count), 0) == line_ref[...]).astype(
        jnp.float32
    )
    to_line = to_line.astype(low)
    residual = (
        lax.dot_general(
            to_line,
            arrived_ref[:, :LANES],
            (((0,), (0,)), ((), ())),
            preferred_element_type=jnp.float32,
        )[:, :columns]
        - targets_ref[...]
    )
    residual_ref[...] = residual
    residual = residual.astype(low)
    coefficient = lax.dot_general(
        arrived_ref[:, LANES:],
        dot(to_line, residual).astype(low),
        (((0,), (0,)), ((), ())),
        preferred_element_type=jnp.float32,
    )
    square = (ranks, ranks)
    diagonal = lax.broadcasted_iota(jnp.int32, square, 0) == lax.broadcasted_iota(
        jnp.int32, square, 1
    )
    scale = jnp.sum(jnp.where(diagonal, scale_ref[...], 0.0), axis=1, keepdims=True)
    correction = (step_size * scale * coefficient).astype(low)
    updated_ref[...] = (
        weights_ref[...]
        + dot(sub_vecs_ref[...], correction)
        - step_size * dot(batch_spread_ref[...], residual)
    )


def body(centers, weights, targets, batch_rows, subsample, eigvecs, eig_scale):
    low = jnp.bfloat16
    row_count, feature_count = centers.shape
    nout, nctr = lax.axis_size(OUT), lax.axis_size(CTR)
    nx, nz = lax.axis_size("x"), lax.axis_size("z")
    ny, ncore = lax.axis_size("y"), lax.axis_size("core")
    place, slice_at = lax.axis_index(CTR), lax.axis_index(OUT)
    batch = batch_rows.shape[0]
    columns = weights.shape[1]
    block = batch // nout
    base = place * row_count

    edges = jnp.arange(nctr, dtype=jnp.int32)[:, None] * row_count
    owned = (batch_rows[None, :] >= edges) & (batch_rows[None, :] < edges + row_count)
    most = jnp.max(jnp.sum(owned.astype(jnp.int32), axis=1))
    batch_line = batch_rows[None, :]

    def places(turn):
        return jnp.stack([place, slice_at, jnp.int32(turn * ROUND), jnp.int32(nout)])

    def round_of(turn):
        at = places(turn)
        shape = jax.ShapeDtypeStruct((ROUND, feature_count), low)
        share = whole(pick_kernel, shape, 2)(at, batch_line, centers)
        arrived = copied_to_all(share.reshape(-1, LANES), CTR)
        arrived = arrived.reshape(nctr * ROUND, feature_count)
        shape = jax.ShapeDtypeStruct((block, feature_count), low)
        slot = functools.partial(slot_kernel, count=row_count)
        return whole(slot, shape, 2)(at, batch_line, arrived)

    def more(carry):
        return carry[0] * (ROUND * nout) < most

    def next_round(carry):
        return carry[0] + 1, carry[1] + round_of(carry[0])

    feats = round_of(0)
    _, feats = lax.while_loop(more, next_round, (jnp.int32(1), feats))

    weights_low = jnp.pad(weights.astype(low), ((0, 0), (0, LANES - columns)))
    mine = jnp.stack(
        [weights_low]
        + [
            lax.ppermute(weights_low, "y", [(i, (i + dy) % ny) for i in range(ny)])
            for dy in range(1, ny)
        ]
    )
    other = lax.ppermute(mine, "core", [(i, (i + 1) % ncore) for i in range(ncore)])

    sub_vecs = dot(one_hot_columns(subsample - base, row_count), eigvecs).astype(low)
    right_norm = jnp.sum(jnp.square(centers.astype(jnp.float32)), axis=1)
    parts = products(places(0), feats, centers, right_norm[None, :], mine, other, sub_vecs)

    blocks = parts.shape[1] // LANES
    arrived = exchanged(parts.reshape(nctr, blocks // 4, 4, LANES), CTR)
    share = arrived.astype(jnp.float32).sum(axis=0).astype(low)
    share = copied_to_all(share, "z").reshape(nz, blocks, LANES)
    heads = jnp.moveaxis(share[:, :nout], 1, 0).reshape(ncore, ny, nz, LANES)
    heads = by_owner(by_owner(heads, 0, "core"), 1, "y")
    heads = jnp.moveaxis(heads, 0, 1).reshape(nout, nz, LANES)
    tails = share[:, nout:].reshape(nz, -1)
    pieces = jnp.concatenate([heads, jnp.broadcast_to(tails, (nout, *tails.shape))], axis=2)
    pieces = jnp.broadcast_to(pieces[:, None], (nout, nx, *pieces.shape[1:]))
    arrived = exchanged(pieces.reshape(nout * nx, *pieces.shape[2:]), (*OUT, "x"))
    arrived = arrived.reshape(batch, -1)

    rank = jnp.sum((batch_rows[None, :] < batch_rows[:, None]).astype(jnp.int32), axis=1)
    slot = rank // nout
    line = (rank % nout) * block + (slot % nx) * nz + slot // nx
    batch_spread = one_hot_columns(batch_rows - base, row_count)
    shapes = (
        jax.ShapeDtypeStruct(weights.shape, jnp.float32),
        jax.ShapeDtypeStruct(targets.shape, jnp.float32),
    )
    return whole(tail_kernel, shapes, 7)(
        places(0),
        arrived,
        line[None, :],
        eig_scale[None, :],
        sub_vecs,
        batch_spread,
        weights,
        targets,
    )


def solution(mesh):
    axes = ("y", "core", "z", "x")
    fine = Mesh(mesh.devices.reshape(4, 2, 16, 4), axes)
    placed = (P(CTR, None), P(CTR, OUT), P(None, OUT), P(), P(CTR), P(CTR, None), P())
    return jax.shard_map(
        body,
        mesh=fine,
        in_specs=placed,
        out_specs=(P(CTR, OUT), P(None, OUT)),
        check_vma=False,
    )
```

```python
import functools
import jax
import jax.numpy as jnp
from jax import lax
from jax.experimental import pallas as pl
from jax.experimental.pallas import tpu as pltpu
from jax.sharding import Mesh, PartitionSpec as P

step_size = 0.5
OUT = ("y", "core")
CTR = ("z", "x")
LANES = 128
ROUND = 3


def exchanged(pieces, axes):
    return lax.all_to_all(pieces, axes, split_axis=0, concat_axis=0, tiled=True)


def copied_to_all(shard, axes):
    return exchanged(jnp.broadcast_to(shard, (lax.axis_size(axes), *shard.shape)), axes)


def one_hot_columns(rows, length):
    return (lax.broadcasted_iota(jnp.int32, (length, rows.shape[0]), 0) == rows[None, :]).astype(
        jnp.bfloat16
    )


def dot(left, right):
    return jnp.dot(left, right, preferred_element_type=jnp.float32)


def by_owner(blocks, dim, name):
    size = lax.axis_size(name)
    back = jnp.concatenate([lax.rev(blocks, (dim,))] * 2, axis=dim)
    return lax.dynamic_slice_in_dim(back, size - 1 - lax.axis_index(name), size, axis=dim)


def whole(kernel, shape, count):
    vmem = pl.BlockSpec(memory_space=pltpu.VMEM)
    return pl.pallas_call(
        kernel,
        out_shape=shape,
        in_specs=[pl.BlockSpec(memory_space=pltpu.SMEM)] + [vmem] * count,
        out_specs=jax.tree.map(lambda _: vmem, shape),
        compiler_params=pltpu.CompilerParams(vmem_limit_bytes=12 << 20),
    )


def rows_below(rows, edge):
    return jnp.sum((rows < edge).astype(jnp.float32), axis=1, keepdims=True).astype(jnp.int32)


def pick_kernel(at_ref, rows_ref, centers_ref, out_ref):
    count = centers_ref.shape[0]
    base, slice_at, step, nout = at_ref[0] * count, at_ref[1], at_ref[2], at_ref[3]
    rows = rows_ref[...]
    here = lax.broadcasted_iota(jnp.int32, (count, 1), 0) + base
    start = rows_below(rows, jnp.full((1, 1), base, jnp.int32))
    lead = start + ((slice_at - start) & (nout - 1))
    held = jnp.sum((rows == here).astype(jnp.float32), axis=1, keepdims=True) > 0
    position = jnp.where(held, rows_below(rows, here), -1)
    steps = lax.broadcasted_iota(jnp.int32, (1, LANES), 1)
    wanted = jnp.where(steps < ROUND, lead + (steps + step) * nout, -2)
    pick = (position == wanted).astype(jnp.float32).astype(jnp.bfloat16)
    found = lax.dot_general(
        pick, centers_ref[...], (((0,), (0,)), ((), ())), preferred_element_type=jnp.float32
    )
    out_ref[...] = found[: out_ref.shape[0]].astype(jnp.bfloat16)


def slot_kernel(at_ref, rows_ref, arrived_ref, out_ref, *, count):
    slice_at, step, nout = at_ref[1], at_ref[2], at_ref[3]
    rows = rows_ref[...]
    line = lax.broadcasted_iota(jnp.int32, (arrived_ref.shape[0], 1), 0)
    scale = (1 << 16) // ROUND + 1
    place = (line * scale) >> 16
    start = rows_below(rows, place * count)
    stop = rows_below(rows, place * count + count)
    lead = start + ((slice_at - start) & (nout - 1))
    position = lead + (line - place * ROUND + step) * nout
    slots = lax.broadcasted_iota(jnp.int32, (1, LANES), 1) * nout + slice_at
    fits = (jnp.where(position < stop, position, -1) == slots).astype(jnp.float32)
    feats = lax.dot_general(
        fits.astype(jnp.bfloat16),
        arrived_ref[...],
        (((0,), (0,)), ((), ())),
        preferred_element_type=jnp.float32,
    )
    out_ref[...] = feats[: out_ref.shape[0]].astype(jnp.bfloat16)


def products_kernel(at_ref, feats_ref, centers_ref, norm_ref, mine_ref, other_ref, vecs_ref, out_ref):
    del at_ref
    low = jnp.bfloat16
    feats = feats_ref[...]
    wide = feats.astype(jnp.float32)
    left_norm = jnp.sum(wide * wide, axis=1, keepdims=True)
    inner = lax.dot_general(
        feats, centers_ref[...], (((1,), (1,)), ((), ())), preferred_element_type=jnp.float32
    )
    kernel = jnp.exp(
        -(left_norm + norm_ref[...] - 2.0 * inner) * (2.0 / feats.shape[1])
    ).astype(low)
    at = 0
    for blocks in (mine_ref, other_ref):
        for j in range(blocks.shape[0]):
            out_ref[:, at : at + LANES] = dot(kernel, blocks[j]).astype(low)
            at += LANES
    out_ref[:, at:] = dot(kernel, vecs_ref[...]).astype(low)


def products(at, feats, centers, norm, mine, other, vecs):
    width = (mine.shape[0] + other.shape[0]) * LANES + vecs.shape[1]
    shape = jax.ShapeDtypeStruct((feats.shape[0], width), jnp.bfloat16)
    return whole(products_kernel, shape, 6)(
        at, feats, centers, norm, mine, other, vecs
    )


def tail_kernel(
    at_ref,
    arrived_ref,
    line_ref,
    scale_ref,
    sub_vecs_ref,
    batch_spread_ref,
    weights_ref,
    targets_ref,
    updated_ref,
    residual_ref,
):
    del at_ref
    low = jnp.bfloat16
    columns = weights_ref.shape[1]
    count, ranks = line_ref.shape[1], scale_ref.shape[1]
    to_line = (lax.broadcasted_iota(jnp.int32, (count, count), 0) == line_ref[...]).astype(
        jnp.float32
    )
    to_line = to_line.astype(low)
    residual = (
        lax.dot_general(
            to_line,
            arrived_ref[:, :LANES],
            (((0,), (0,)), ((), ())),
            preferred_element_type=jnp.float32,
        )[:, :columns]
        - targets_ref[...]
    )
    residual_ref[...] = residual
    residual = residual.astype(low)
    coefficient = lax.dot_general(
        arrived_ref[:, LANES:],
        dot(to_line, residual).astype(low),
        (((0,), (0,)), ((), ())),
        preferred_element_type=jnp.float32,
    )
    square = (ranks, ranks)
    diagonal = lax.broadcasted_iota(jnp.int32, square, 0) == lax.broadcasted_iota(
        jnp.int32, square, 1
    )
    scale = jnp.sum(jnp.where(diagonal, scale_ref[...], 0.0), axis=1, keepdims=True)
    correction = (step_size * scale * coefficient).astype(low)
    updated_ref[...] = (
        weights_ref[...]
        + dot(sub_vecs_ref[...], correction)
        - step_size * dot(batch_spread_ref[...], residual)
    )


def body(centers, weights, targets, batch_rows, subsample, eigvecs, eig_scale):
    low = jnp.bfloat16
    row_count, feature_count = centers.shape
    nout, nctr = lax.axis_size(OUT), lax.axis_size(CTR)
    nx, nz = lax.axis_size("x"), lax.axis_size("z")
    ny, ncore = lax.axis_size("y"), lax.axis_size("core")
    place, slice_at = lax.axis_index(CTR), lax.axis_index(OUT)
    batch = batch_rows.shape[0]
    columns = weights.shape[1]
    block = batch // nout
    base = place * row_count

    edges = jnp.arange(nctr, dtype=jnp.int32)[:, None] * row_count
    owned = (batch_rows[None, :] >= edges) & (batch_rows[None, :] < edges + row_count)
    most = jnp.max(jnp.sum(owned.astype(jnp.int32), axis=1))
    batch_line = batch_rows[None, :]

    def places(turn):
        return jnp.stack([place, slice_at, jnp.int32(turn * ROUND), jnp.int32(nout)])

    def round_of(turn):
        at = places(turn)
        shape = jax.ShapeDtypeStruct((ROUND, feature_count), low)
        share = whole(pick_kernel, shape, 2)(at, batch_line, centers)
        arrived = copied_to_all(share.reshape(-1, LANES), CTR)
        arrived = arrived.reshape(nctr * ROUND, feature_count)
        shape = jax.ShapeDtypeStruct((block, feature_count), low)
        slot = functools.partial(slot_kernel, count=row_count)
        return whole(slot, shape, 2)(at, batch_line, arrived)

    def more(carry):
        return carry[0] * (ROUND * nout) < most

    def next_round(carry):
        return carry[0] + 1, carry[1] + round_of(carry[0])

    feats = round_of(0)
    _, feats = lax.while_loop(more, next_round, (jnp.int32(1), feats))

    weights_low = jnp.pad(weights.astype(low), ((0, 0), (0, LANES - columns)))
    ring = [[(i, (i + dy) % ny) for i in range(ny)] for dy in range(ny)]
    two = lax.ppermute(weights_low, "y", ring[2])
    one, three = (lax.ppermute(weights_low, "y", ring[dy]) for dy in (1, 3))
    mine = jnp.stack([weights_low, one, two, three])
    other = lax.ppermute(mine, "core", [(i, (i + 1) % ncore) for i in range(ncore)])

    sub_vecs = dot(one_hot_columns(subsample - base, row_count), eigvecs).astype(low)
    right_norm = jnp.sum(jnp.square(centers.astype(jnp.float32)), axis=1)
    parts = products(places(0), feats, centers, right_norm[None, :], mine, other, sub_vecs)

    blocks = parts.shape[1] // LANES
    arrived = exchanged(parts.reshape(nctr, blocks // 4, 4, LANES), CTR)
    share = arrived.astype(jnp.float32).sum(axis=0).astype(low)
    share = copied_to_all(share, "z").reshape(nz, blocks, LANES)
    heads = jnp.moveaxis(share[:, :nout], 1, 0).reshape(ncore, ny, nz, LANES)
    heads = by_owner(by_owner(heads, 0, "core"), 1, "y")
    heads = jnp.moveaxis(heads, 0, 1).reshape(nout, nz, LANES)
    tails = share[:, nout:].reshape(nz, -1)
    pieces = jnp.concatenate([heads, jnp.broadcast_to(tails, (nout, *tails.shape))], axis=2)
    pieces = jnp.broadcast_to(pieces[:, None], (nout, nx, *pieces.shape[1:]))
    arrived = exchanged(pieces.reshape(nout * nx, *pieces.shape[2:]), (*OUT, "x"))
    arrived = arrived.reshape(batch, -1)

    rank = jnp.sum((batch_rows[None, :] < batch_rows[:, None]).astype(jnp.int32), axis=1)
    slot = rank // nout
    line = (rank % nout) * block + (slot % nx) * nz + slot // nx
    batch_spread = one_hot_columns(batch_rows - base, row_count)
    shapes = (
        jax.ShapeDtypeStruct(weights.shape, jnp.float32),
        jax.ShapeDtypeStruct(targets.shape, jnp.float32),
    )
    return whole(tail_kernel, shapes, 7)(
        places(0),
        arrived,
        line[None, :],
        eig_scale[None, :],
        sub_vecs,
        batch_spread,
        weights,
        targets,
    )


def solution(mesh):
    axes = ("y", "core", "z", "x")
    fine = Mesh(mesh.devices.reshape(4, 2, 16, 4), axes)
    placed = (P(CTR, None), P(CTR, OUT), P(None, OUT), P(), P(CTR), P(CTR, None), P())
    return jax.shard_map(
        body,
        mesh=fine,
        in_specs=placed,
        out_specs=(P(CTR, OUT), P(None, OUT)),
        check_vma=False,
    )
```

```python
import functools
import jax
import jax.numpy as jnp
from jax import lax
from jax.experimental import pallas as pl
from jax.experimental.pallas import tpu as pltpu
from jax.sharding import Mesh, PartitionSpec as P

step_size = 0.5
OUT = ("y", "core")
CTR = ("z", "x")
LANES = 128
ROUND = 3


def exchanged(pieces, axes):
    return lax.all_to_all(pieces, axes, split_axis=0, concat_axis=0, tiled=True)


def one_hot_columns(rows, length):
    return (lax.broadcasted_iota(jnp.int32, (length, rows.shape[0]), 0) == rows[None, :]).astype(
        jnp.bfloat16
    )


def dot(left, right):
    return jnp.dot(left, right, preferred_element_type=jnp.float32)


def by_owner(blocks, dim, name):
    size = lax.axis_size(name)
    back = jnp.concatenate([lax.rev(blocks, (dim,))] * 2, axis=dim)
    return lax.dynamic_slice_in_dim(back, size - 1 - lax.axis_index(name), size, axis=dim)


def whole(kernel, shape, count):
    vmem = pl.BlockSpec(memory_space=pltpu.VMEM)
    return pl.pallas_call(
        kernel,
        out_shape=shape,
        in_specs=[pl.BlockSpec(memory_space=pltpu.SMEM)] + [vmem] * count,
        out_specs=jax.tree.map(lambda _: vmem, shape),
        compiler_params=pltpu.CompilerParams(vmem_limit_bytes=12 << 20),
    )


def rows_below(rows, edge):
    return jnp.sum((rows < edge).astype(jnp.float32), axis=1, keepdims=True).astype(jnp.int32)


def pick_kernel(at_ref, rows_ref, centers_ref, out_ref, norm_ref, most_ref, *, nctr):
    count = centers_ref.shape[0]
    base, slice_at, step, nout = at_ref[0] * count, at_ref[1], at_ref[2], at_ref[3]
    rows = rows_ref[...]
    here = lax.broadcasted_iota(jnp.int32, (count, 1), 0) + base
    start = rows_below(rows, jnp.full((1, 1), base, jnp.int32))
    lead = start + ((slice_at - start) & (nout - 1))
    held = jnp.sum((rows == here).astype(jnp.float32), axis=1, keepdims=True) > 0
    position = jnp.where(held, rows_below(rows, here), -1)
    steps = lax.broadcasted_iota(jnp.int32, (1, LANES), 1)
    wanted = jnp.where(steps < ROUND, lead + (steps + step) * nout, -2)
    pick = (position == wanted).astype(jnp.float32).astype(jnp.bfloat16)
    found = lax.dot_general(
        pick, centers_ref[...], (((0,), (0,)), ((), ())), preferred_element_type=jnp.float32
    )
    out_ref[...] = found[: out_ref.shape[0]].astype(jnp.bfloat16)
    wide = centers_ref[...].astype(jnp.float32)
    norm = jnp.sum(wide * wide, axis=1, keepdims=True)
    norm_ref[...] = jnp.transpose(jnp.broadcast_to(norm, (count, LANES)))[:1]
    edges = lax.broadcasted_iota(jnp.int32, (nctr, 1), 0) * count
    most = jnp.max(rows_below(rows, edges + count) - rows_below(rows, edges), axis=0, keepdims=True)
    most_ref[...] = most


def slot_kernel(at_ref, rows_ref, arrived_ref, out_ref, *, count):
    slice_at, step, nout = at_ref[1], at_ref[2], at_ref[3]
    rows = rows_ref[...]
    line = lax.broadcasted_iota(jnp.int32, (arrived_ref.shape[0], 1), 0)
    scale = (1 << 16) // ROUND + 1
    place = (line * scale) >> 16
    start = rows_below(rows, place * count)
    stop = rows_below(rows, place * count + count)
    lead = start + ((slice_at - start) & (nout - 1))
    position = lead + (line - place * ROUND + step) * nout
    slots = lax.broadcasted_iota(jnp.int32, (1, LANES), 1) * nout + slice_at
    fits = (jnp.where(position < stop, position, -1) == slots).astype(jnp.float32)
    feats = lax.dot_general(
        fits.astype(jnp.bfloat16),
        arrived_ref[...],
        (((0,), (0,)), ((), ())),
        preferred_element_type=jnp.float32,
    )
    out_ref[...] = feats[: out_ref.shape[0]].astype(jnp.bfloat16)


def products_kernel(at_ref, feats_ref, centers_ref, norm_ref, mine_ref, other_ref, vecs_ref, out_ref):
    del at_ref
    low = jnp.bfloat16
    feats = feats_ref[...]
    wide = feats.astype(jnp.float32)
    left_norm = jnp.sum(wide * wide, axis=1, keepdims=True)
    inner = lax.dot_general(
        feats, centers_ref[...], (((1,), (1,)), ((), ())), preferred_element_type=jnp.float32
    )
    kernel = jnp.exp(
        -(left_norm + norm_ref[...] - 2.0 * inner) * (2.0 / feats.shape[1])
    ).astype(low)
    at = 0
    for blocks in (mine_ref, other_ref):
        for j in range(blocks.shape[0]):
            out_ref[:, at : at + LANES] = dot(kernel, blocks[j]).astype(low)
            at += LANES
    out_ref[:, at:] = dot(kernel, vecs_ref[...]).astype(low)


def products(at, feats, centers, norm, mine, other, vecs):
    width = (mine.shape[0] + other.shape[0]) * LANES + vecs.shape[1]
    shape = jax.ShapeDtypeStruct((feats.shape[0], width), jnp.bfloat16)
    return whole(products_kernel, shape, 6)(
        at, feats, centers, norm, mine, other, vecs
    )


def tail_kernel(
    at_ref,
    arrived_ref,
    line_ref,
    scale_ref,
    sub_vecs_ref,
    batch_spread_ref,
    weights_ref,
    targets_ref,
    updated_ref,
    residual_ref,
):
    del at_ref
    low = jnp.bfloat16
    columns = weights_ref.shape[1]
    count, ranks = line_ref.shape[1], scale_ref.shape[1]
    to_line = (lax.broadcasted_iota(jnp.int32, (count, count), 0) == line_ref[...]).astype(
        jnp.float32
    )
    to_line = to_line.astype(low)
    residual = (
        lax.dot_general(
            to_line,
            arrived_ref[:, :LANES],
            (((0,), (0,)), ((), ())),
            preferred_element_type=jnp.float32,
        )[:, :columns]
        - targets_ref[...]
    )
    residual_ref[...] = residual
    residual = residual.astype(low)
    coefficient = lax.dot_general(
        arrived_ref[:, LANES:],
        dot(to_line, residual).astype(low),
        (((0,), (0,)), ((), ())),
        preferred_element_type=jnp.float32,
    )
    square = (ranks, ranks)
    diagonal = lax.broadcasted_iota(jnp.int32, square, 0) == lax.broadcasted_iota(
        jnp.int32, square, 1
    )
    scale = jnp.sum(jnp.where(diagonal, scale_ref[...], 0.0), axis=1, keepdims=True)
    correction = (step_size * scale * coefficient).astype(low)
    updated_ref[...] = (
        weights_ref[...]
        + dot(sub_vecs_ref[...], correction)
        - step_size * dot(batch_spread_ref[...], residual)
    )


def body(centers, weights, targets, batch_rows, subsample, eigvecs, eig_scale):
    low = jnp.bfloat16
    row_count, feature_count = centers.shape
    nout, nctr = lax.axis_size(OUT), lax.axis_size(CTR)
    nx, nz = lax.axis_size("x"), lax.axis_size("z")
    ny, ncore = lax.axis_size("y"), lax.axis_size("core")
    place, slice_at = lax.axis_index(CTR), lax.axis_index(OUT)
    batch = batch_rows.shape[0]
    columns = weights.shape[1]
    block = batch // nout
    base = place * row_count

    batch_line = batch_rows[None, :]

    def places(turn):
        return jnp.stack([place, slice_at, jnp.int32(turn * ROUND), jnp.int32(nout)])

    def round_of(turn):
        at = places(turn)
        shapes = (
            jax.ShapeDtypeStruct((ROUND, feature_count), low),
            jax.ShapeDtypeStruct((1, row_count), jnp.float32),
            jax.ShapeDtypeStruct((1, 1), jnp.int32),
        )
        pick = functools.partial(pick_kernel, nctr=nctr)
        share, norm, most = whole(pick, shapes, 2)(at, batch_line, centers)
        arrived = lax.all_gather(share.reshape(-1, LANES), CTR, axis=0, tiled=True)
        arrived = arrived.reshape(nctr * ROUND, feature_count)
        shape = jax.ShapeDtypeStruct((block, feature_count), low)
        slot = functools.partial(slot_kernel, count=row_count)
        return whole(slot, shape, 2)(at, batch_line, arrived), norm, most

    feats, right_norm, most = round_of(0)
    most = most[0, 0]

    def more(carry):
        return carry[0] * (ROUND * nout) < most

    def next_round(carry):
        return carry[0] + 1, carry[1] + round_of(carry[0])[0]

    _, feats = lax.while_loop(more, next_round, (jnp.int32(1), feats))

    weights_low = jnp.pad(weights.astype(low), ((0, 0), (0, LANES - columns)))
    mine = jnp.stack(
        [weights_low]
        + [
            lax.ppermute(weights_low, "y", [(i, (i + dy) % ny) for i in range(ny)])
            for dy in range(1, ny)
        ]
    )
    other = lax.ppermute(mine, "core", [(i, (i + 1) % ncore) for i in range(ncore)])

    sub_vecs = dot(one_hot_columns(subsample - base, row_count), eigvecs).astype(low)
    parts = products(places(0), feats, centers, right_norm, mine, other, sub_vecs)

    blocks = parts.shape[1] // LANES
    arrived = exchanged(parts.reshape(nctr, blocks // 4, 4, LANES), CTR)
    share = arrived.astype(jnp.float32).sum(axis=0).astype(low)
    share = lax.all_gather(share.reshape(blocks, LANES), "z", axis=0)
    heads = jnp.moveaxis(share[:, :nout], 1, 0).reshape(ncore, ny, nz, LANES)
    heads = by_owner(by_owner(heads, 0, "core"), 1, "y")
    heads = jnp.moveaxis(heads, 0, 1).reshape(nout, nz, LANES)
    tails = share[:, nout:].reshape(nz, -1)
    pieces = jnp.concatenate([heads, jnp.broadcast_to(tails, (nout, *tails.shape))], axis=2)
    pieces = jnp.broadcast_to(pieces[:, None], (nout, nx, *pieces.shape[1:]))
    arrived = exchanged(pieces.reshape(nout * nx, *pieces.shape[2:]), (*OUT, "x"))
    arrived = arrived.reshape(batch, -1)

    rank = jnp.sum((batch_rows[None, :] < batch_rows[:, None]).astype(jnp.int32), axis=1)
    slot = rank // nout
    line = (rank % nout) * block + (slot % nx) * nz + slot // nx
    batch_spread = one_hot_columns(batch_rows - base, row_count)
    shapes = (
        jax.ShapeDtypeStruct(weights.shape, jnp.float32),
        jax.ShapeDtypeStruct(targets.shape, jnp.float32),
    )
    return whole(tail_kernel, shapes, 7)(
        places(0),
        arrived,
        line[None, :],
        eig_scale[None, :],
        sub_vecs,
        batch_spread,
        weights,
        targets,
    )


def solution(mesh):
    axes = ("y", "core", "z", "x")
    fine = Mesh(mesh.devices.reshape(4, 2, 16, 4), axes)
    placed = (P(CTR, None), P(CTR, OUT), P(None, OUT), P(), P(CTR), P(CTR, None), P())
    return jax.shard_map(
        body,
        mesh=fine,
        in_specs=placed,
        out_specs=(P(CTR, OUT), P(None, OUT)),
        check_vma=False,
    )
```

```python
import functools
import jax
import jax.numpy as jnp
from jax import lax
from jax.experimental import pallas as pl
from jax.experimental.pallas import tpu as pltpu
from jax.sharding import Mesh, PartitionSpec as P

step_size = 0.5
OUT = ("y", "core")
CTR = ("z", "x")
LANES = 128
ROUND = 3


def exchanged(pieces, axes):
    return lax.all_to_all(pieces, axes, split_axis=0, concat_axis=0, tiled=True)


def copied_to_all(shard, axes):
    return exchanged(jnp.broadcast_to(shard, (lax.axis_size(axes), *shard.shape)), axes)


def one_hot_columns(rows, length):
    return (lax.broadcasted_iota(jnp.int32, (length, rows.shape[0]), 0) == rows[None, :]).astype(
        jnp.bfloat16
    )


def dot(left, right):
    return jnp.dot(left, right, preferred_element_type=jnp.float32)


def by_owner(blocks, dim, name):
    size = lax.axis_size(name)
    back = jnp.concatenate([lax.rev(blocks, (dim,))] * 2, axis=dim)
    return lax.dynamic_slice_in_dim(back, size - 1 - lax.axis_index(name), size, axis=dim)


def whole(kernel, shape, count, left=0, scratch=()):
    vmem = pl.BlockSpec(memory_space=pltpu.VMEM)
    hbm = pl.BlockSpec(memory_space=pltpu.HBM)
    return pl.pallas_call(
        kernel,
        out_shape=shape,
        in_specs=[pl.BlockSpec(memory_space=pltpu.SMEM)] + [vmem] * count + [hbm] * left,
        scratch_shapes=scratch,
        out_specs=jax.tree.map(lambda _: vmem, shape),
        compiler_params=pltpu.CompilerParams(vmem_limit_bytes=12 << 20),
    )


def rows_below(rows, edge):
    return jnp.sum((rows < edge).astype(jnp.float32), axis=1, keepdims=True).astype(jnp.int32)


def pick_kernel(at_ref, rows_ref, centers_ref, out_ref, norm_ref, most_ref, *, nctr):
    count = centers_ref.shape[0]
    base, slice_at, step, nout = at_ref[0] * count, at_ref[1], at_ref[2], at_ref[3]
    rows = rows_ref[...]
    here = lax.broadcasted_iota(jnp.int32, (count, 1), 0) + base
    start = rows_below(rows, jnp.full((1, 1), base, jnp.int32))
    lead = start + ((slice_at - start) & (nout - 1))
    held = jnp.sum((rows == here).astype(jnp.float32), axis=1, keepdims=True) > 0
    position = jnp.where(held, rows_below(rows, here), -1)
    steps = lax.broadcasted_iota(jnp.int32, (1, LANES), 1)
    wanted = jnp.where(steps < ROUND, lead + (steps + step) * nout, -2)
    pick = (position == wanted).astype(jnp.float32).astype(jnp.bfloat16)
    found = lax.dot_general(
        pick, centers_ref[...], (((0,), (0,)), ((), ())), preferred_element_type=jnp.float32
    )
    out_ref[...] = found[: out_ref.shape[0]].astype(jnp.bfloat16)
    wide = centers_ref[...].astype(jnp.float32)
    norm = jnp.sum(wide * wide, axis=1, keepdims=True)
    norm_ref[...] = jnp.transpose(jnp.broadcast_to(norm, (count, LANES)))[:1]
    edges = lax.broadcasted_iota(jnp.int32, (nctr, 1), 0) * count
    most = jnp.max(rows_below(rows, edges + count) - rows_below(rows, edges), axis=0, keepdims=True)
    most_ref[...] = most


def slot_kernel(at_ref, rows_ref, arrived_ref, out_ref, *, count):
    slice_at, step, nout = at_ref[1], at_ref[2], at_ref[3]
    rows = rows_ref[...]
    line = lax.broadcasted_iota(jnp.int32, (arrived_ref.shape[0], 1), 0)
    scale = (1 << 16) // ROUND + 1
    place = (line * scale) >> 16
    start = rows_below(rows, place * count)
    stop = rows_below(rows, place * count + count)
    lead = start + ((slice_at - start) & (nout - 1))
    position = lead + (line - place * ROUND + step) * nout
    slots = lax.broadcasted_iota(jnp.int32, (1, LANES), 1) * nout + slice_at
    fits = (jnp.where(position < stop, position, -1) == slots).astype(jnp.float32)
    feats = lax.dot_general(
        fits.astype(jnp.bfloat16),
        arrived_ref[...],
        (((0,), (0,)), ((), ())),
        preferred_element_type=jnp.float32,
    )
    out_ref[...] = feats[: out_ref.shape[0]].astype(jnp.bfloat16)


def products_kernel(at_ref, feats_ref, centers_ref, norm_ref, mine_ref, other_ref, vecs_ref, out_ref):
    del at_ref
    low = jnp.bfloat16
    feats = feats_ref[...]
    wide = feats.astype(jnp.float32)
    left_norm = jnp.sum(wide * wide, axis=1, keepdims=True)
    inner = lax.dot_general(
        feats, centers_ref[...], (((1,), (1,)), ((), ())), preferred_element_type=jnp.float32
    )
    kernel = jnp.exp(
        -(left_norm + norm_ref[...] - 2.0 * inner) * (2.0 / feats.shape[1])
    ).astype(low)
    at = 0
    for blocks in (mine_ref, other_ref):
        for j in range(blocks.shape[0]):
            out_ref[:, at : at + LANES] = dot(kernel, blocks[j]).astype(low)
            at += LANES
    out_ref[:, at:] = dot(kernel, vecs_ref[...]).astype(low)


def products(at, feats, centers, norm, mine, other, vecs):
    width = (mine.shape[0] + other.shape[0]) * LANES + vecs.shape[1]
    shape = jax.ShapeDtypeStruct((feats.shape[0], width), jnp.bfloat16)
    return whole(products_kernel, shape, 6)(
        at, feats, centers, norm, mine, other, vecs
    )


def tail_kernel(
    at_ref,
    arrived_ref,
    line_ref,
    scale_ref,
    sub_vecs_ref,
    batch_spread_ref,
    targets_ref,
    weights_ref,
    updated_ref,
    residual_ref,
    held_ref,
    done,
):
    del at_ref
    fetch = pltpu.make_async_copy(weights_ref, held_ref, done)
    fetch.start()
    low = jnp.bfloat16
    columns = weights_ref.shape[1]
    count, ranks = line_ref.shape[1], scale_ref.shape[1]
    to_line = (lax.broadcasted_iota(jnp.int32, (count, count), 0) == line_ref[...]).astype(
        jnp.float32
    )
    to_line = to_line.astype(low)
    residual = (
        lax.dot_general(
            to_line,
            arrived_ref[:, :LANES],
            (((0,), (0,)), ((), ())),
            preferred_element_type=jnp.float32,
        )[:, :columns]
        - targets_ref[...]
    )
    residual_ref[...] = residual
    residual = residual.astype(low)
    coefficient = lax.dot_general(
        arrived_ref[:, LANES:],
        dot(to_line, residual).astype(low),
        (((0,), (0,)), ((), ())),
        preferred_element_type=jnp.float32,
    )
    square = (ranks, ranks)
    diagonal = lax.broadcasted_iota(jnp.int32, square, 0) == lax.broadcasted_iota(
        jnp.int32, square, 1
    )
    scale = jnp.sum(jnp.where(diagonal, scale_ref[...], 0.0), axis=1, keepdims=True)
    correction = (step_size * scale * coefficient).astype(low)
    fetch.wait()
    updated_ref[...] = (
        held_ref[...]
        + dot(sub_vecs_ref[...], correction)
        - step_size * dot(batch_spread_ref[...], residual)
    )


def body(centers, weights, targets, batch_rows, subsample, eigvecs, eig_scale):
    low = jnp.bfloat16
    row_count, feature_count = centers.shape
    nout, nctr = lax.axis_size(OUT), lax.axis_size(CTR)
    nx, nz = lax.axis_size("x"), lax.axis_size("z")
    ny, ncore = lax.axis_size("y"), lax.axis_size("core")
    place, slice_at = lax.axis_index(CTR), lax.axis_index(OUT)
    batch = batch_rows.shape[0]
    columns = weights.shape[1]
    block = batch // nout
    base = place * row_count

    batch_line = batch_rows[None, :]

    def places(turn):
        return jnp.stack([place, slice_at, jnp.int32(turn * ROUND), jnp.int32(nout)])

    def round_of(turn):
        at = places(turn)
        shapes = (
            jax.ShapeDtypeStruct((ROUND, feature_count), low),
            jax.ShapeDtypeStruct((1, row_count), jnp.float32),
            jax.ShapeDtypeStruct((1, 1), jnp.int32),
        )
        pick = functools.partial(pick_kernel, nctr=nctr)
        share, norm, most = whole(pick, shapes, 2)(at, batch_line, centers)
        arrived = copied_to_all(share.reshape(-1, LANES), CTR)
        arrived = arrived.reshape(nctr * ROUND, feature_count)
        shape = jax.ShapeDtypeStruct((block, feature_count), low)
        slot = functools.partial(slot_kernel, count=row_count)
        return whole(slot, shape, 2)(at, batch_line, arrived), norm, most

    feats, right_norm, most = round_of(0)
    most = most[0, 0]

    def more(carry):
        return carry[0] * (ROUND * nout) < most

    def next_round(carry):
        return carry[0] + 1, carry[1] + round_of(carry[0])[0]

    _, feats = lax.while_loop(more, next_round, (jnp.int32(1), feats))

    weights_low = jnp.pad(weights.astype(low), ((0, 0), (0, LANES - columns)))
    ahead = [(i, (i + 1) % ny) for i in range(ny)]
    back = [(i, (i - 1) % ny) for i in range(ny)]
    one, three = lax.ppermute(weights_low, "y", ahead), lax.ppermute(weights_low, "y", back)
    two = lax.ppermute(one, "y", ahead)
    mine = jnp.stack([weights_low, one, two, three])
    other = lax.ppermute(mine, "core", [(i, (i + 1) % ncore) for i in range(ncore)])

    sub_vecs = dot(one_hot_columns(subsample - base, row_count), eigvecs).astype(low)
    parts = products(places(0), feats, centers, right_norm, mine, other, sub_vecs)

    blocks = parts.shape[1] // LANES
    arrived = exchanged(parts.reshape(nctr, blocks // 4, 4, LANES), CTR)
    share = arrived.astype(jnp.float32).sum(axis=0).astype(low)
    share = copied_to_all(share, "z").reshape(nz, blocks, LANES)
    heads = jnp.moveaxis(share[:, :nout], 1, 0).reshape(ncore, ny, nz, LANES)
    heads = by_owner(by_owner(heads, 0, "core"), 1, "y")
    heads = jnp.moveaxis(heads, 0, 1).reshape(nout, nz, LANES)
    tails = share[:, nout:].reshape(nz, -1)
    pieces = jnp.concatenate([heads, jnp.broadcast_to(tails, (nout, *tails.shape))], axis=2)
    pieces = jnp.broadcast_to(pieces[:, None], (nout, nx, *pieces.shape[1:]))
    arrived = exchanged(pieces.reshape(nout * nx, *pieces.shape[2:]), (*OUT, "x"))
    arrived = arrived.reshape(batch, -1)

    rank = jnp.sum((batch_rows[None, :] < batch_rows[:, None]).astype(jnp.int32), axis=1)
    slot = rank // nout
    line = (rank % nout) * block + (slot % nx) * nz + slot // nx
    batch_spread = one_hot_columns(batch_rows - base, row_count)
    shapes = (
        jax.ShapeDtypeStruct(weights.shape, jnp.float32),
        jax.ShapeDtypeStruct(targets.shape, jnp.float32),
    )
    scratch = (pltpu.VMEM(weights.shape, jnp.float32), pltpu.SemaphoreType.DMA)
    return whole(tail_kernel, shapes, 6, 1, scratch)(
        places(0),
        arrived,
        line[None, :],
        eig_scale[None, :],
        sub_vecs,
        batch_spread,
        targets,
        weights,
    )


def solution(mesh):
    axes = ("y", "core", "z", "x")
    fine = Mesh(mesh.devices.reshape(4, 2, 16, 4), axes)
    placed = (P(CTR, None), P(CTR, OUT), P(None, OUT), P(), P(CTR), P(CTR, None), P())
    return jax.shard_map(
        body,
        mesh=fine,
        in_specs=placed,
        out_specs=(P(CTR, OUT), P(None, OUT)),
        check_vma=False,
    )
```

```python
import functools
import jax
import jax.numpy as jnp
from jax import lax
from jax.experimental import pallas as pl
from jax.experimental.pallas import tpu as pltpu
from jax.sharding import Mesh, PartitionSpec as P

step_size = 0.5
OUT = ("y", "core")
CTR = ("z", "x")
LANES = 128
ROUND = 3


def exchanged(pieces, axes):
    return lax.all_to_all(pieces, axes, split_axis=0, concat_axis=0, tiled=True)


def copied_to_all(shard, axes):
    return exchanged(jnp.broadcast_to(shard, (lax.axis_size(axes), *shard.shape)), axes)


def one_hot(rows, length):
    return (lax.broadcasted_iota(jnp.int32, (rows.shape[0], length), 1) == rows[:, None]).astype(
        jnp.bfloat16
    )


def one_hot_columns(rows, length):
    return (lax.broadcasted_iota(jnp.int32, (length, rows.shape[0]), 0) == rows[None, :]).astype(
        jnp.bfloat16
    )


def dot(left, right):
    return jnp.dot(left, right, preferred_element_type=jnp.float32)


def by_owner(blocks, dim, name):
    size = lax.axis_size(name)
    back = jnp.concatenate([lax.rev(blocks, (dim,))] * 2, axis=dim)
    return lax.dynamic_slice_in_dim(back, size - 1 - lax.axis_index(name), size, axis=dim)


def whole(kernel, shape, count):
    vmem = pl.BlockSpec(memory_space=pltpu.VMEM)
    return pl.pallas_call(
        kernel,
        out_shape=shape,
        in_specs=[pl.BlockSpec(memory_space=pltpu.SMEM)] + [vmem] * count,
        out_specs=jax.tree.map(lambda _: vmem, shape),
        compiler_params=pltpu.CompilerParams(vmem_limit_bytes=12 << 20),
    )


def rows_below(rows, edge):
    return jnp.sum((rows < edge).astype(jnp.float32), axis=1, keepdims=True).astype(jnp.int32)


def pick_kernel(at_ref, rows_ref, centers_ref, out_ref, norm_ref, most_ref, *, nctr):
    count = centers_ref.shape[0]
    base, slice_at, step, nout = at_ref[0] * count, at_ref[1], at_ref[2], at_ref[3]
    rows = rows_ref[...]
    here = lax.broadcasted_iota(jnp.int32, (count, 1), 0) + base
    start = rows_below(rows, jnp.full((1, 1), base, jnp.int32))
    lead = start + ((slice_at - start) & (nout - 1))
    held = jnp.sum((rows == here).astype(jnp.float32), axis=1, keepdims=True) > 0
    position = jnp.where(held, rows_below(rows, here), -1)
    steps = lax.broadcasted_iota(jnp.int32, (1, LANES), 1)
    wanted = jnp.where(steps < ROUND, lead + (steps + step) * nout, -2)
    pick = (position == wanted).astype(jnp.float32).astype(jnp.bfloat16)
    found = lax.dot_general(
        pick, centers_ref[...], (((0,), (0,)), ((), ())), preferred_element_type=jnp.float32
    )
    out_ref[...] = found[: out_ref.shape[0]].astype(jnp.bfloat16)
    wide = centers_ref[...].astype(jnp.float32)
    norm = jnp.sum(wide * wide, axis=1, keepdims=True)
    norm_ref[...] = jnp.transpose(jnp.broadcast_to(norm, (count, LANES)))[:1]
    edges = lax.broadcasted_iota(jnp.int32, (nctr, 1), 0) * count
    most = jnp.max(rows_below(rows, edges + count) - rows_below(rows, edges), axis=0, keepdims=True)
    most_ref[...] = most


def slot_kernel(at_ref, rows_ref, arrived_ref, out_ref, *, count):
    slice_at, step, nout = at_ref[1], at_ref[2], at_ref[3]
    rows = rows_ref[...]
    line = lax.broadcasted_iota(jnp.int32, (arrived_ref.shape[0], 1), 0)
    scale = (1 << 16) // ROUND + 1
    place = (line * scale) >> 16
    start = rows_below(rows, place * count)
    stop = rows_below(rows, place * count + count)
    lead = start + ((slice_at - start) & (nout - 1))
    position = lead + (line - place * ROUND + step) * nout
    slots = lax.broadcasted_iota(jnp.int32, (1, LANES), 1) * nout + slice_at
    fits = (jnp.where(position < stop, position, -1) == slots).astype(jnp.float32)
    feats = lax.dot_general(
        fits.astype(jnp.bfloat16),
        arrived_ref[...],
        (((0,), (0,)), ((), ())),
        preferred_element_type=jnp.float32,
    )
    out_ref[...] = feats[: out_ref.shape[0]].astype(jnp.bfloat16)


def products_kernel(at_ref, feats_ref, centers_ref, norm_ref, mine_ref, other_ref, vecs_ref, out_ref):
    del at_ref
    low = jnp.bfloat16
    feats = feats_ref[...]
    wide = feats.astype(jnp.float32)
    left_norm = jnp.sum(wide * wide, axis=1, keepdims=True)
    inner = lax.dot_general(
        feats, centers_ref[...], (((1,), (1,)), ((), ())), preferred_element_type=jnp.float32
    )
    kernel = jnp.exp(
        -(left_norm + norm_ref[...] - 2.0 * inner) * (2.0 / feats.shape[1])
    ).astype(low)
    at = 0
    for blocks in (mine_ref, other_ref):
        for j in range(blocks.shape[0]):
            out_ref[:, at : at + LANES] = dot(kernel, blocks[j]).astype(low)
            at += LANES
    out_ref[:, at:] = dot(kernel, vecs_ref[...]).astype(low)


def products(at, feats, centers, norm, mine, other, vecs):
    width = (mine.shape[0] + other.shape[0]) * LANES + vecs.shape[1]
    shape = jax.ShapeDtypeStruct((feats.shape[0], width), jnp.bfloat16)
    return whole(products_kernel, shape, 6)(
        at, feats, centers, norm, mine, other, vecs
    )


def body(centers, weights, targets, batch_rows, subsample, eigvecs, eig_scale):
    low = jnp.bfloat16
    row_count, feature_count = centers.shape
    nout, nctr = lax.axis_size(OUT), lax.axis_size(CTR)
    nx, nz = lax.axis_size("x"), lax.axis_size("z")
    ny, ncore = lax.axis_size("y"), lax.axis_size("core")
    place, slice_at = lax.axis_index(CTR), lax.axis_index(OUT)
    batch = batch_rows.shape[0]
    columns = weights.shape[1]
    block = batch // nout
    base = place * row_count

    batch_line = batch_rows[None, :]

    def places(turn):
        return jnp.stack([place, slice_at, jnp.int32(turn * ROUND), jnp.int32(nout)])

    def round_of(turn):
        at = places(turn)
        shapes = (
            jax.ShapeDtypeStruct((ROUND, feature_count), low),
            jax.ShapeDtypeStruct((1, row_count), jnp.float32),
            jax.ShapeDtypeStruct((1, 1), jnp.int32),
        )
        pick = functools.partial(pick_kernel, nctr=nctr)
        share, norm, most = whole(pick, shapes, 2)(at, batch_line, centers)
        arrived = copied_to_all(share.reshape(-1, LANES), CTR)
        arrived = arrived.reshape(nctr * ROUND, feature_count)
        shape = jax.ShapeDtypeStruct((block, feature_count), low)
        slot = functools.partial(slot_kernel, count=row_count)
        return whole(slot, shape, 2)(at, batch_line, arrived), norm, most

    feats, right_norm, most = round_of(0)
    most = most[0, 0]

    def more(carry):
        return carry[0] * (ROUND * nout) < most

    def next_round(carry):
        return carry[0] + 1, carry[1] + round_of(carry[0])[0]

    _, feats = lax.while_loop(more, next_round, (jnp.int32(1), feats))

    weights_low = jnp.pad(weights.astype(low), ((0, 0), (0, LANES - columns)))
    mine = jnp.stack(
        [weights_low]
        + [
            lax.ppermute(weights_low, "y", [(i, (i + dy) % ny) for i in range(ny)])
            for dy in range(1, ny)
        ]
    )
    other = lax.ppermute(mine, "core", [(i, (i + 1) % ncore) for i in range(ncore)])

    sub_vecs = dot(one_hot_columns(subsample - base, row_count), eigvecs).astype(low)
    parts = products(places(0), feats, centers, right_norm, mine, other, sub_vecs)

    blocks = parts.shape[1] // LANES
    arrived = exchanged(parts.reshape(nctr, blocks // 4, 4, LANES), CTR)
    share = arrived.astype(jnp.float32).sum(axis=0).astype(low)
    share = copied_to_all(share, "z").reshape(nz, blocks, LANES)
    heads = jnp.moveaxis(share[:, :nout], 1, 0).reshape(ncore, ny, nz, LANES)
    heads = by_owner(by_owner(heads, 0, "core"), 1, "y")
    heads = jnp.moveaxis(heads, 0, 1).reshape(nout, nz, LANES)
    tails = share[:, nout:].reshape(nz, -1)
    pieces = jnp.concatenate([heads, jnp.broadcast_to(tails, (nout, *tails.shape))], axis=2)
    pieces = jnp.broadcast_to(pieces[:, None], (nout, nx, *pieces.shape[1:]))
    arrived = exchanged(pieces.reshape(nout * nx, *pieces.shape[2:]), (*OUT, "x"))
    arrived = arrived.reshape(batch, -1)

    rank = jnp.sum((batch_rows[None, :] < batch_rows[:, None]).astype(jnp.int32), axis=1)
    slot = rank // nout
    line = (rank % nout) * block + (slot % nx) * nz + slot // nx
    to_batch = one_hot(line, batch)
    line_rows = jnp.sum(
        jnp.where(
            lax.broadcasted_iota(jnp.int32, (batch, batch), 0) == line[None, :],
            batch_rows[None, :],
            0,
        ),
        axis=1,
    )
    line_targets = lax.dot_general(
        to_batch.astype(jnp.float32),
        targets,
        (((0,), (0,)), ((), ())),
        precision=lax.Precision.HIGHEST,
    )
    batch_spread = one_hot_columns(line_rows - base, row_count)
    line_targets, batch_spread = lax.optimization_barrier((line_targets, batch_spread))
    spread = jnp.concatenate([sub_vecs, batch_spread], axis=1)

    line_prediction = arrived[:, :columns]
    line_residual = line_prediction.astype(jnp.float32) - line_targets
    coefficient = lax.dot_general(
        arrived[:, LANES:],
        line_residual.astype(low),
        (((0,), (0,)), ((), ())),
        preferred_element_type=jnp.float32,
    )
    changes = jnp.concatenate(
        [
            (step_size * eig_scale[:, None] * coefficient).astype(low),
            (-step_size * line_residual).astype(low),
        ]
    )
    updated = weights + dot(spread, changes)
    residual = dot(to_batch, line_prediction) - targets
    return (updated, residual)


def solution(mesh):
    axes = ("y", "core", "z", "x")
    fine = Mesh(mesh.devices.reshape(4, 2, 16, 4), axes)
    placed = (P(CTR, None), P(CTR, OUT), P(None, OUT), P(), P(CTR), P(CTR, None), P())
    return jax.shard_map(
        body,
        mesh=fine,
        in_specs=placed,
        out_specs=(P(CTR, OUT), P(None, OUT)),
        check_vma=False,
    )
```
